32 devices in a mesh: wrow: 4 (over y, core), wcol: 2 (over x), dom: 4 (over z).
Axes of the slice: x: 2, y: 2, z: 4, core: 2. Of those that a mesh axis runs over, the one named last changes fastest.
Arguments:
- positions: float32 [4, 2, 3, 8192], P('wrow', 'wcol', None, 'dom'), may hold values from -6 to 6
- velocities: float32 [4, 2, 3, 8192], P('wrow', 'wcol', None, 'dom'), may hold values from -6 to 6
- inv_mass: float32 [8192], P('dom'), may hold values from 0.5 to 2
- cv_weight: float32 [2, 3, 8192], P(None, None, 'dom'), may hold values from -0.125 to 0.125
- stiffness: float32 [2], replicated, may hold values from 1 to 4
- centers: float32 [4, 2, 2], P('wrow', 'wcol'), may hold values from -3 to 3
- block_order: int32 [8192], P('dom'), may hold values from 0 to 2047, as said below
- pair_count: int32 [4], P('dom'), may hold values from 16 to 64, as said below
- pair_own: int32 [4, 64], P('dom'), may hold values from 0 to 15, as said below
- pair_other: int32 [4, 64], P('dom'), may hold values from 0 to 47, as said below
- accept_row: int32 [4, 2], P('wrow', 'wcol'), may hold values from 0 to 1, as said below
- accept_col: int32 [4, 2], P('wrow', 'wcol'), may hold values from 0 to 1, as said below
Outputs:
- new_positions: float32 [4, 2, 3, 8192], P('wrow', 'wcol', None, 'dom')
- new_velocities: float32 [4, 2, 3, 8192], P('wrow', 'wcol', None, 'dom')
- new_forces: float32 [4, 2, 3, 8192], P('wrow', 'wcol', None, 'dom')
The draws below stay inside these ranges and needn't reach their ends.
Inputs may be any that keep to these rules, and one draw needn't show every extreme that they name: accept_row is equal for windows (2k, c) and (2k + 1, c). accept_col is equal for windows (r, 2k) and (r, 2k + 1). `block_order`: each slab's 2048 entries are a permutation of 0 to 2047. `pair_count`: some slab has exactly 64 live pairs. `pair_own`: entries past the slab's pair_count are 0. `pair_other`: slab 0 names no lower slab and the last slab no upper slab; entries past the slab's pair_count are 16.
All inputs are finite; a program needn't handle non-finite values.
Results may differ from the reference program's by a relative error of at most 0.0003.
Values sent between devices are 32-bit elements; how exact they have to be, the bound alone decides.
A program may use at most 64 MiB of HBM per device.

```python
import math
import jax
import jax.numpy as jnp
from jax import lax

ATOM_DEV = 2048
BLK = 128
STEPS = 3
NB = 16
PMAX = 64
ATOMS = 8192
NROW = 4
NCOL = 2


def counts_of(key):
    domains = ATOMS // ATOM_DEV
    base = jax.random.randint(jax.random.fold_in(key, 11), (domains,), PMAX // 4, PMAX + 1)
    chosen = jax.random.randint(jax.random.fold_in(key, 12), (), 0, domains)
    return jnp.where(jnp.arange(domains) == chosen, PMAX, base).astype(jnp.int32)


def live_slots(key):
    return jnp.arange(PMAX)[None, :] < counts_of(key)[:, None]


def draw_pair_count(key, part):
    return counts_of(key)


def draw_pair_own(key, part):
    domains = ATOMS // ATOM_DEV
    raw_blocks = jax.random.randint(jax.random.fold_in(key, 13), (domains, PMAX), 0, NB)
    return jnp.where(live_slots(key), raw_blocks, 0).astype(jnp.int32)


def draw_pair_other(key, part):
    domains = ATOMS // ATOM_DEV
    raw_blocks = jax.random.randint(jax.random.fold_in(key, 14), (domains, PMAX), 0, 3 * NB)
    slab_ids = jnp.arange(domains)[:, None]
    raw_blocks = jnp.where((slab_ids == 0) & (raw_blocks < NB), raw_blocks + NB, raw_blocks)
    raw_blocks = jnp.where((slab_ids == domains - 1) & (raw_blocks >= 2 * NB), raw_blocks - NB, raw_blocks)
    return jnp.where(live_slots(key), raw_blocks, NB).astype(jnp.int32)


def draw_block_order(key, part):
    domains = ATOMS // ATOM_DEV

    def one_slab(slab):
        return jax.random.permutation(jax.random.fold_in(key, 31 + slab), ATOM_DEV)
    return jax.vmap(one_slab)(jnp.arange(domains)).reshape(ATOMS).astype(jnp.int32)


def draw_accept_row(key, part):
    halves = jax.random.randint(jax.random.fold_in(key, 21), (NROW // 2, NCOL), 0, 2)
    halves = halves.at[0, 0].set(1).at[0, 1].set(0)
    return jnp.repeat(halves, 2, axis=0).astype(jnp.int32)


def draw_accept_col(key, part):
    halves = jax.random.randint(jax.random.fold_in(key, 22), (NROW, NCOL // 2), 0, 2)
    halves = halves.at[0, 0].set(1).at[1, 0].set(0)
    return jnp.repeat(halves, 2, axis=1).astype(jnp.int32)


def steps_of(stream_key, dims, cuts, smallest, largest):
    loudness = 1.0
    for axis_at, shards_of in cuts:
        heights = jax.random.uniform(jax.random.fold_in(jax.random.fold_in(stream_key, 6), axis_at), (shards_of,), jnp.float32, smallest / len(cuts), largest / len(cuts))
        loudness = loudness * jnp.repeat(jnp.exp(heights), dims[axis_at] // shards_of).reshape((-1,) + (1,) * (len(dims) - 1 - axis_at))
    return loudness


def scatter_about(key, extent, width, most, split=(), held_as=jnp.bfloat16):
    array = width * jax.random.normal(key, extent, jnp.float32)
    if split:
        array = array * steps_of(key, extent, split, -0.22, 0.18)
    return jnp.clip(array, -most, most).astype(held_as)


def setup_inputs(seed: int = 0) -> dict:
    seeds = jax.random.split(jax.random.key(seed), 13)
    return {
        "positions": scatter_about(seeds[0], (NROW, NCOL, 3, ATOMS), 1.0, 6.0, ((0, 4), (1, 2), (3, 4)), jnp.float32),
        "velocities": scatter_about(seeds[1], (NROW, NCOL, 3, ATOMS), 1.0, 6.0, ((0, 4), (1, 2), (3, 4)), jnp.float32),
        "inv_mass": jnp.clip(jnp.exp(math.log(2.0) - 1.3862944 * jax.random.uniform(seeds[2], (ATOMS,), jnp.float32) ** steps_of(seeds[2], (ATOMS,), ((0, 4),), -0.2, 0.2)), 0.5, 2.0),
        "cv_weight": scatter_about(seeds[3], (2, 3, ATOMS), ATOM_DEV ** -0.5, 0.125, ((2, 4),), jnp.float32),
        "stiffness": jnp.clip(jnp.exp(jax.random.uniform(seeds[4], (2,), jnp.float32, math.log(1.0), math.log(4.0))), 1.0, 4.0),
        "centers": jnp.clip(jax.random.uniform(seeds[5], (NROW, NCOL, 2), jnp.float32, -3.0, 3.0) * steps_of(seeds[5], (NROW, NCOL, 2), ((0, 4), (1, 2)), -0.4, 0.0), -3.0, 3.0),
        "block_order": draw_block_order(jax.random.fold_in(seeds[12], 71), 0),
        "pair_count": draw_pair_count(jax.random.fold_in(seeds[12], 71), 0),
        "pair_own": draw_pair_own(jax.random.fold_in(seeds[12], 71), 0),
        "pair_other": draw_pair_other(jax.random.fold_in(seeds[12], 71), 0),
        "accept_row": draw_accept_row(jax.random.fold_in(seeds[12], 71), 0),
        "accept_col": draw_accept_col(jax.random.fold_in(seeds[12], 71), 0),
    }


PAIR_EPS = 0.015625
DT = 0.1


def pair_tile(own_tile, other_tile):
    offsets = own_tile[:, :, None] - other_tile[:, None, :]
    squared = jnp.sum(offsets * offsets, axis=0)
    weight_tile = PAIR_EPS * jnp.exp(-0.5 * squared)
    return own_tile * jnp.sum(weight_tile, axis=1)[None, :] - jnp.dot(other_tile, weight_tile.T, precision=lax.Precision.HIGHEST)


def domain_forces(nearby, pair_total, own_blocks, other_blocks):
    blocks_dev = ATOM_DEV // BLK

    def add_tile(forces_acc, index):
        own_index = own_blocks[index]
        other_index = other_blocks[index]
        own_tile = lax.dynamic_slice(nearby, (jnp.int32(0), ((blocks_dev + own_index) * BLK).astype(jnp.int32)), (3, BLK))
        other_tile = lax.dynamic_slice(nearby, (jnp.int32(0), (other_index * BLK).astype(jnp.int32)), (3, BLK))
        live = (index < pair_total).astype(forces_acc.dtype)
        offset = (own_index * BLK).astype(jnp.int32)
        older = lax.dynamic_slice(forces_acc, (jnp.int32(0), offset), (3, BLK))
        forces_acc = lax.dynamic_update_slice(forces_acc, older + live * pair_tile(own_tile, other_tile), (jnp.int32(0), offset))
        return forces_acc, None

    forces_acc, _ = lax.scan(add_tile, jnp.zeros((3, ATOM_DEV), jnp.float32), jnp.arange(PMAX, dtype=jnp.int32))
    return forces_acc


def window_pair(coords, pair_count, pair_own, pair_other):
    domains = ATOMS // ATOM_DEV
    slab_rows = coords.reshape(3, domains, ATOM_DEV)
    zeros_slab = jnp.zeros((3, 1, ATOM_DEV), coords.dtype)
    padded = jnp.concatenate([zeros_slab, slab_rows, zeros_slab], axis=1)
    nearby = jnp.stack([padded[:, slab:slab + 3].reshape(3, 3 * ATOM_DEV) for slab in range(domains)])
    forces_all = jax.vmap(domain_forces)(nearby, pair_count, pair_own, pair_other)
    return jnp.transpose(forces_all, (1, 0, 2)).reshape(3, ATOMS)


def total_force(coords, weights, stiffness, centre_rows, pair_count, pair_own, pair_other):
    pair = jax.vmap(window_pair, in_axes=(0, None, None, None))(coords, pair_count, pair_own, pair_other)
    collective = jnp.sum(weights[None] * coords[:, None], axis=(2, 3))
    pull = stiffness[None, :] * (collective - centre_rows)
    return pair - jnp.sum(pull[:, :, None, None] * weights[None], axis=1)


def partner_select(state, flags, axis):
    count_axis = state.shape[axis]
    swapped = jnp.take(state, jnp.arange(count_axis, dtype=jnp.int32) ^ 1, axis=axis)
    return jnp.where((flags == 1)[:, :, None, None], swapped, state)


def reference(positions, velocities, inv_mass, cv_weight, stiffness, centers, block_order, pair_count, pair_own, pair_other, accept_row, accept_col):
    domains = ATOMS // ATOM_DEV
    windows = NROW * NCOL
    global_order = (block_order.reshape(domains, ATOM_DEV) + (jnp.arange(domains, dtype=jnp.int32) * ATOM_DEV)[:, None]).reshape(ATOMS).astype(jnp.int32)
    inverse = jnp.zeros((ATOMS,), jnp.int32).at[global_order].set(jnp.arange(ATOMS, dtype=jnp.int32))
    coords = positions.reshape(windows, 3, ATOMS)[:, :, global_order]
    speeds = velocities.reshape(windows, 3, ATOMS)[:, :, global_order]
    inverse_mass = inv_mass[global_order]
    weights = cv_weight[:, :, global_order]
    centre_rows = centers.reshape(windows, 2)
    forces_now = total_force(coords, weights, stiffness, centre_rows, pair_count, pair_own, pair_other)
    for _ in range(STEPS):
        speeds = speeds + (0.5 * DT) * inverse_mass * forces_now
        coords = coords + DT * speeds
        forces_now = total_force(coords, weights, stiffness, centre_rows, pair_count, pair_own, pair_other)
        speeds = speeds + (0.5 * DT) * inverse_mass * forces_now
    results = []
    for state in (coords, speeds, forces_now):
        state = state[:, :, inverse].reshape(NROW, NCOL, 3, ATOMS)
        state = partner_select(state, accept_row, 0)
        state = partner_select(state, accept_col, 1)
        results.append(state)
    return (results[0], results[1], results[2])
```

```python
import functools
import math

import numpy as np
import jax
import jax.numpy as jnp
from jax import lax
from jax.experimental import pallas as pl
from jax.experimental.pallas import tpu as pltpu
from jax.sharding import PartitionSpec as P

BLK = 128
STEPS = 3
PAIR_EPS = 0.015625
DT = 0.1
SCALE = math.sqrt(math.log2(math.e))
ROWS = 32
UNROLL = 16
OTHER_ROWS = {0: 0, 1: 1, 2: 2, 3: 3, 4: 4, 5: 5, 6: 9, 7: 9, 8: 9, 9: 6, 10: 7, 11: 8, 16: 0, 17: 1, 18: 2, 19: 3, 20: 4, 21: 5}
OWN_ROWS = {0: 0, 1: 1, 2: 2, 3: 0, 4: 1, 5: 2, 6: 6, 7: 7, 8: 8, 9: 9, 10: 9, 11: 9, 16: 3, 17: 4, 18: 5, 19: 3, 20: 4, 21: 5}
MESH = pl.DeviceIdType.MESH
F32 = jnp.float32
BF16 = jnp.bfloat16


def split3(value):
    high = value.astype(BF16)
    rest = value - high.astype(F32)
    middle = rest.astype(BF16)
    low = (rest - middle.astype(F32)).astype(BF16)
    return high, middle, low


def stacked_split(value):
    return jnp.concatenate(split3(value), axis=0)


def unsplit(value, rows):
    return value[0:rows] + (value[rows : 2 * rows] + value[2 * rows : 3 * rows])


def placing(rows_of, nb):
    table = np.zeros((nb, ROWS, 10, nb), np.float32)
    for row, kind in rows_of.items():
        for b in range(nb):
            table[b, row, kind, b] = 1.0
    return jnp.asarray(table.reshape(nb * ROWS, 10 * nb), BF16)


def kernel(
    sizes,
    pos, vel, mass, cvw, order, own_row, place_own, place_other, own_s, other_s, count_s, stiff_s, centers_s, arow_s, acol_s,
    out_x, out_v, out_f,
    onehot, high_block, raw, raw_w, got_x, got_v, got_aux, aux, parts, tiles, others_of, turned_own, summing, xs, vs, fs, ms, ws,
    sx_send, sx_recv, sv_send, sv_recv, sa_send, sa_recv, halo_send, halo_recv, part_send, part_recv, *nears,
):
    doms, nb, slots = sizes
    row = lax.axis_index("wrow")
    col = lax.axis_index("wcol")
    me = lax.axis_index("dom")
    row_to = row + 1 - 2 * lax.rem(row, 2)
    col_to = col + 1 - 2 * lax.rem(col, 2)
    partners = [(row_to, col, me), (row, col_to, me), (row_to, col_to, me)]
    others = [(row, col, lax.rem(me + off, doms)) for off in range(1, doms)]

    lines = lax.broadcasted_iota(jnp.int32, (8, BLK), 0)
    aux[...] = jnp.where(
        lines == 0,
        centers_s[0, 0],
        jnp.where(lines == 1, centers_s[0, 1], arow_s[0, 0].astype(F32)),
    )
    for held in nears:
        held[...] = jnp.zeros(held.shape, F32)
    barrier = pltpu.get_barrier_semaphore()
    for target in partners + others:
        pl.semaphore_signal(barrier, inc=1, device_id=target, device_id_type=MESH)
    pl.semaphore_wait(barrier, len(partners) + len(others))

    def exchange(source, target, sends, recvs):
        copies = []
        for at, partner in enumerate(partners):
            copy = pltpu.make_async_remote_copy(
                src_ref=source,
                dst_ref=target.at[at],
                send_sem=sends.at[at],
                recv_sem=recvs.at[at],
                device_id=partner,
                device_id_type=MESH,
            )
            copy.start()
            copies.append(copy)
        return copies

    aux_copies = exchange(aux, got_aux, sa_send, sa_recv)
    x_copies = exchange(pos, got_x, sx_send, sx_recv)
    v_copies = exchange(vel, got_v, sv_send, sv_recv)

    jl = lax.broadcasted_iota(jnp.int32, (BLK, BLK), 0)
    listed = order[...]
    low = lax.rem(listed, BLK)
    high_block[...] = lax.div(listed, BLK)
    for b in range(nb):
        onehot[:, b * BLK : (b + 1) * BLK] = jnp.where(low[b : b + 1, :] == jl, 1.0, 0.0).astype(BF16)
    jb_lines = lax.broadcasted_iota(jnp.int32, (nb, BLK), 0)

    def permuted(source, comps, store):
        split = stacked_split(source)

        def body(b, carry):
            at = pl.ds(pl.multiple_of(b * BLK, BLK), BLK)
            picked = jnp.dot(split, onehot[:, at], preferred_element_type=F32)
            picked = unsplit(picked, comps * nb)
            mask = high_block[pl.ds(b, 1), :] == jb_lines
            for k in range(comps):
                line = jnp.sum(jnp.where(mask, picked[k * nb : (k + 1) * nb], 0.0), axis=0, keepdims=True)
                store(k, b, line)
            return carry

        lax.fori_loop(0, nb, body, 0, unroll=True)

    def unpermuted(source_ref):
        def body(b, total):
            at = pl.ds(pl.multiple_of(b * BLK, BLK), BLK)
            mask = high_block[pl.ds(b, 1), :] == jb_lines
            spread = jnp.concatenate(
                [jnp.where(mask, source_ref[k, pl.ds(b, 1), :], 0.0) for k in range(3)], axis=0
            )
            return total + lax.dot_general(
                stacked_split(spread), onehot[:, at], (((1,), (1,)), ((), ())), preferred_element_type=F32
            )

        total = lax.fori_loop(0, nb, body, jnp.zeros((9 * nb, BLK), F32), unroll=True)
        return unsplit(total, 3 * nb).reshape(3, nb, BLK)

    for k in range(2):
        for c in range(3):
            raw_w[(3 * k + c) * nb : (3 * k + c + 1) * nb, :] = cvw[pl.ds(2 * nb * c + k, nb, stride=2), :]
    raw_w[6 * nb : 7 * nb, :] = mass[...]

    def store_w(k, b, line):
        if k < 6:
            ws[k // 3, k % 3, pl.ds(b, 1), :] = line
        else:
            ms[pl.ds(b, 1), :] = line

    permuted(raw_w[...], 7, store_w)

    wide = 8 * slots
    at_slot = lax.div(lax.broadcasted_iota(jnp.int32, (slots, wide), 1), 8)
    spread_slots = jnp.where(at_slot == lax.broadcasted_iota(jnp.int32, (slots, wide), 0), 1.0, 0.0).astype(BF16)
    live = lax.broadcasted_iota(jnp.int32, (8, slots), 1) < count_s[0]
    owners = jnp.where(live, jnp.broadcast_to(own_row[...], (8, slots)).astype(F32), -1.0).astype(BF16)
    owners = jnp.dot(owners, spread_slots, preferred_element_type=F32)[0:1, :]
    block_line = lax.broadcasted_iota(jnp.int32, (nb, wide), 0).astype(F32)
    row_line = lax.rem(lax.broadcasted_iota(jnp.int32, (nb, wide), 1), 8)
    for r in range(7):
        summing[r * nb : (r + 1) * nb, :] = jnp.where(
            (owners == block_line) & (row_line == r), 1.0, 0.0
        ).astype(BF16)

    for copy in aux_copies:
        copy.wait()
    take_row = jnp.full((8, BLK), arow_s[0, 0].astype(F32)) > 0.5
    take_col = jnp.full((8, BLK), acol_s[0, 0].astype(F32)) > 0.5
    take_far = jnp.broadcast_to(got_aux[1, 2:3, :], (8, BLK)) > 0.5

    def chosen(mine, by_row, by_col, by_both):
        far = jnp.where(take_far, by_both, by_col)
        close = jnp.where(take_row, by_row, mine)
        return jnp.where(take_col, far, close)

    centre = chosen(aux[...], got_aux[0], got_aux[1], got_aux[2])
    centres = [centre[0:1, :], centre[1:2, :]]

    def take_window(source, got):
        for c in range(3):
            for b in range(0, nb, 8):
                raw[c * nb + b : c * nb + b + 8, :] = chosen(
                    source[c, b : b + 8], got[0, c, b : b + 8], got[1, c, b : b + 8], got[2, c, b : b + 8]
                )

    for copy in x_copies:
        copy.wait()
    take_window(pos, got_x)

    def store_x(k, b, line):
        xs[k, pl.ds(b, 1), :] = line

    def store_v(k, b, line):
        vs[k, pl.ds(b, 1), :] = line

    permuted(raw[...], 3, store_x)

    def take_velocities():
        for copy in v_copies:
            copy.wait()
        take_window(vel, got_v)
        permuted(raw[...], 3, store_v)

    def force(e, meanwhile):
        near = nears[e]
        x = xs[...]
        near[1] = x * SCALE
        up = pltpu.make_async_remote_copy(
            src_ref=near.at[1],
            dst_ref=near.at[0],
            send_sem=halo_send.at[e, 0],
            recv_sem=halo_recv.at[e, 0],
            device_id=(row, col, lax.rem(me + 1, doms)),
            device_id_type=MESH,
        )
        down = pltpu.make_async_remote_copy(
            src_ref=near.at[1],
            dst_ref=near.at[2],
            send_sem=halo_send.at[e, 1],
            recv_sem=halo_recv.at[e, 1],
            device_id=(row, col, lax.rem(me + doms - 1, doms)),
            device_id_type=MESH,
        )

        @pl.when(me < doms - 1)
        def _():
            up.start()

        @pl.when(me > 0)
        def _():
            down.start()

        for k in range(2):
            part = jnp.sum(ws[k] * x, axis=0)
            parts[e, me, k] = jnp.sum(part.reshape(nb // 8, 8, BLK), axis=0)
        part_copies = []
        for at, target in enumerate(others):
            copy = pltpu.make_async_remote_copy(
                src_ref=parts.at[e, me],
                dst_ref=parts.at[e, me],
                send_sem=part_send.at[e, at],
                recv_sem=part_recv.at[e, at],
                device_id=target,
                device_id_type=MESH,
            )
            copy.start()
            part_copies.append(copy)

        def features(slab):
            highs, middles, held = [], [], []
            for k in range(3):
                value = near[slab, k]
                high = value.astype(BF16)
                middle = (value - high.astype(F32)).astype(BF16)
                highs.append(high)
                middles.append(middle)
                held.append(high.astype(F32) + middle.astype(F32))
            norm = -0.5 * (held[0] * held[0] + held[1] * held[1] + held[2] * held[2])
            ones = jnp.ones((nb, BLK), BF16)
            return jnp.concatenate(highs + middles + list(split3(norm)) + [ones], axis=0), held

        def place_others(slab, kinds):
            placed = jnp.dot(place_other[...], kinds, preferred_element_type=F32).astype(BF16)
            others_of[slab * nb : (slab + 1) * nb] = placed.reshape(nb, ROWS, BLK)

        kinds, held = features(1)
        place_others(1, kinds)
        placed = jnp.dot(place_own[...], kinds, preferred_element_type=F32)
        for b in range(nb):
            turned_own[b] = jnp.transpose(placed[b * ROWS : (b + 1) * ROWS]).astype(BF16)

        meanwhile()

        @pl.when(me < doms - 1)
        def _():
            up.wait_send()
            down.wait_recv()

        @pl.when(me > 0)
        def _():
            down.wait_send()
            up.wait_recv()

        place_others(0, features(0)[0])
        place_others(2, features(2)[0])

        def first_of(p):
            theirs = others_of[other_s[0, p]]
            return theirs, jnp.dot(turned_own[own_s[0, p]], theirs, preferred_element_type=F32)

        def second_of(p, theirs, logit):
            weight = jnp.exp2(logit)
            high = weight.astype(BF16)
            low = (weight - high.astype(F32)).astype(BF16)
            lines_of = theirs[0:16, :]
            pulled = lax.dot_general(
                jnp.concatenate([lines_of, lines_of], axis=1),
                jnp.concatenate([high, low], axis=1),
                (((1,), (1,)), ((), ())),
                preferred_element_type=F32,
            )
            tiles[p] = pulled[0:8, :]

        def slots_at(first):
            held_of = [first_of(first + u) for u in range(8)]
            for g in range(0, 32, 8):
                later = [first_of(first + g + 8 + u) for u in range(8)] if g + 8 < 32 else []
                for u in range(8):
                    second_of(first + g + u, *held_of[u])
                held_of = later

        def body(i, carry):
            slots_at(i * 32)
            return carry

        lax.fori_loop(0, slots // 32, body, 0)

        for copy in part_copies:
            copy.wait()
        sums = parts[e, 0]
        for d in range(1, doms):
            sums = sums + parts[e, d]
        pulls = []
        for k in range(2):
            collective = jnp.sum(sums[k], axis=(0, 1), keepdims=True)
            pulls.append(stiff_s[k] * (collective - centres[k]))
        total = sum(
            jnp.dot(summing[...], term, preferred_element_type=F32)
            for term in split3(tiles[...].reshape(8 * slots, BLK))[::-1]
        )
        for k in range(3):
            pulled = total[k * nb : (k + 1) * nb] + total[(3 + k) * nb : (4 + k) * nb]
            pair = held[k] * total[6 * nb : 7 * nb] - pulled
            fs[k] = (PAIR_EPS / SCALE) * pair - pulls[0] * ws[0, k] - pulls[1] * ws[1, k]

    force(0, take_velocities)
    for step in range(STEPS):
        half = 0.5 * DT * ms[...]
        for k in range(3):
            v = vs[k] + half * fs[k]
            vs[k] = v
            xs[k] = xs[k] + DT * v
        if step < STEPS - 1:
            force(step + 1, lambda: None)
            for k in range(3):
                vs[k] = vs[k] + half * fs[k]

    def write_positions():
        out_x[...] = unpermuted(xs)
        out_v[...] = unpermuted(vs)

    force(STEPS, write_positions)
    forces = unpermuted(fs)
    out_f[...] = forces
    out_v[...] = out_v[...] + (0.5 * DT) * mass[...][None] * forces


def per_device(
    positions, velocities, inv_mass, cv_weight, stiffness, centers, block_order, pair_count, pair_own, pair_other,
    accept_row, accept_col,
):
    atoms = block_order.shape[0]
    nb = atoms // BLK
    slots = pair_own.shape[1]
    doms = lax.axis_size("dom")
    evals = STEPS + 1
    vmem = pl.BlockSpec(memory_space=pltpu.VMEM)
    smem = pl.BlockSpec(memory_space=pltpu.SMEM)
    dma = pltpu.SemaphoreType.DMA
    shape = jax.ShapeDtypeStruct((3, nb, BLK), F32)
    weights = cv_weight.transpose(1, 0, 2).reshape(3, 2, nb, BLK).transpose(0, 2, 1, 3).reshape(6 * nb, BLK)
    outs = pl.pallas_call(
        functools.partial(kernel, (doms, nb, slots)),
        out_shape=(shape, shape, shape),
        in_specs=[vmem] * 8 + [smem] * 7,
        out_specs=(vmem, vmem, vmem),
        scratch_shapes=[
            pltpu.VMEM((BLK, atoms), BF16),
            pltpu.VMEM((nb, BLK), jnp.int32),
            pltpu.VMEM((3 * nb, BLK), F32),
            pltpu.VMEM((7 * nb, BLK), F32),
            pltpu.VMEM((3, 3, nb, BLK), F32),
            pltpu.VMEM((3, 3, nb, BLK), F32),
            pltpu.VMEM((3, 8, BLK), F32),
            pltpu.VMEM((8, BLK), F32),
            pltpu.VMEM((evals, doms, 2, 8, BLK), F32),
            pltpu.VMEM((slots, 8, BLK), F32),
            pltpu.VMEM((3 * nb, ROWS, BLK), BF16),
            pltpu.VMEM((nb, BLK, ROWS), BF16),
            pltpu.VMEM((7 * nb, 8 * slots), BF16),
            pltpu.VMEM((3, nb, BLK), F32),
            pltpu.VMEM((3, nb, BLK), F32),
            pltpu.VMEM((3, nb, BLK), F32),
            pltpu.VMEM((nb, BLK), F32),
            pltpu.VMEM((2, 3, nb, BLK), F32),
            dma((3,)), dma((3,)), dma((3,)), dma((3,)), dma((3,)), dma((3,)),
            dma((evals, 2)), dma((evals, 2)), dma((evals, doms)), dma((evals, doms)),
        ]
        + [pltpu.VMEM((3, 3, nb, BLK), F32)] * evals,
        compiler_params=pltpu.CompilerParams(collective_id=0, has_side_effects=True),
        name="windows",
    )(
        positions.reshape(3, nb, BLK), velocities.reshape(3, nb, BLK), inv_mass.reshape(nb, BLK), weights, block_order.reshape(nb, BLK), pair_own,
        placing(OWN_ROWS, nb), placing(OTHER_ROWS, nb), pair_own, pair_other, pair_count, stiffness, centers[0], accept_row, accept_col,
    )
    return tuple(out.reshape(1, 1, 3, atoms) for out in outs)


def solution(mesh):
    placed = (
        P("wrow", "wcol", None, "dom"),
        P("wrow", "wcol", None, "dom"),
        P("dom"),
        P(None, None, "dom"),
        P(),
        P("wrow", "wcol", None),
        P("dom"),
        P("dom"),
        P("dom", None),
        P("dom", None),
        P("wrow", "wcol"),
        P("wrow", "wcol"),
    )
    return jax.shard_map(
        per_device,
        mesh=mesh,
        in_specs=placed,
        out_specs=(
            P("wrow", "wcol", None, "dom"),
            P("wrow", "wcol", None, "dom"),
            P("wrow", "wcol", None, "dom"),
        ),
        check_vma=False,
    )
```

```python
import functools
import math

import jax
import jax.numpy as jnp
from jax import lax
from jax.experimental import pallas as pl
from jax.experimental.pallas import tpu as pltpu
from jax.sharding import PartitionSpec as P

BLK = 128
SUB = 8
STEPS = 3
PAIR_EPS = 0.015625
DT = 0.1
SCALE = math.sqrt(math.log2(math.e))
GROUP = 8
UNROLL = 64
MESH = pl.DeviceIdType.MESH
F32 = jnp.float32
BF16 = jnp.bfloat16
I32 = jnp.int32


def split2(value):
    high = value.astype(BF16)
    return high, (value - high.astype(F32)).astype(BF16)


def kernel(
    sizes,
    pos, vel, mass, cvw, order, own_row, other_row, count_s, stiff_s, centers_s, arow_s, acol_s,
    out_x, out_v, out_f,
    hot, hot_back, block_of, block_back, raw, raw_w, got_x, got_v, got_aux, aux, parts, prefix, lines_of, turned_of, own_of,
    table_i, table_f, list_s, keep_s, xs, vs, fs, held, half_m, ws,
    sx_send, sx_recv, sv_send, sv_recv, sa_send, sa_recv, halo_send, halo_recv, part_send, part_recv, list_sem, *nears,
):
    doms, nb, slots = sizes
    rows = nb * SUB
    row = lax.axis_index("wrow")
    col = lax.axis_index("wcol")
    me = lax.axis_index("dom")
    row_to = row + 1 - 2 * lax.rem(row, 2)
    col_to = col + 1 - 2 * lax.rem(col, 2)
    partners = [(row_to, col, me), (row, col_to, me), (row_to, col_to, me)]
    others = [(row, col, lax.rem(me + off, doms)) for off in range(1, doms)]

    lines = lax.broadcasted_iota(I32, (SUB, BLK), 0)
    aux[...] = jnp.where(
        lines == 0,
        centers_s[0, 0],
        jnp.where(lines == 1, centers_s[0, 1], arow_s[0, 0].astype(F32)),
    )
    barrier = pltpu.get_barrier_semaphore()
    for target in partners + others:
        pl.semaphore_signal(barrier, inc=1, device_id=target, device_id_type=MESH)
    pl.semaphore_wait(barrier, len(partners) + len(others))

    def exchange(source, target, sends, recvs):
        copies = []
        for at, partner in enumerate(partners):
            copy = pltpu.make_async_remote_copy(
                src_ref=source,
                dst_ref=target.at[at],
                send_sem=sends.at[at],
                recv_sem=recvs.at[at],
                device_id=partner,
                device_id_type=MESH,
            )
            copy.start()
            copies.append(copy)
        return copies

    aux_copies = exchange(aux, got_aux, sa_send, sa_recv)
    x_copies = exchange(pos, got_x, sx_send, sx_recv)
    v_copies = exchange(vel, got_v, sv_send, sv_recv)

    lane_line = lax.broadcasted_iota(I32, (BLK, BLK), 0)

    def spread(low, target):
        for b in range(nb):
            target[:, b * BLK : (b + 1) * BLK] = jnp.where(low[b : b + 1, :] == lane_line, 1.0, 0.0).astype(BF16)

    listed = order[...]
    block_of[...] = lax.div(listed, BLK)
    spread(lax.rem(listed, BLK), hot)

    def moved(source, hots, blocks):
        left = jnp.concatenate(split2(source), axis=1)
        for b in range(0, nb, 2):
            right = hots[:, b * BLK : (b + 2) * BLK]
            got = jnp.dot(left, jnp.concatenate([right, right], axis=0), preferred_element_type=F32)
            for u in range(2):
                home = jnp.broadcast_to(blocks[b + u : b + u + 1, :], (SUB, BLK))
                line = got[0:SUB, u * BLK : (u + 1) * BLK]
                for s in range(1, nb):
                    line = jnp.where(home == s, got[s * SUB : (s + 1) * SUB, u * BLK : (u + 1) * BLK], line)
                yield b + u, line

    raw[...] = jnp.zeros((rows, BLK), F32)
    raw_w[...] = jnp.zeros((rows, BLK), F32)
    for k in range(2):
        for c in range(3):
            raw_w[pl.ds(3 * k + c, nb, stride=SUB), :] = cvw[pl.ds(2 * nb * c + k, nb, stride=2), :]
    raw_w[pl.ds(6, nb, stride=SUB), :] = mass[...]
    three = lines < 3
    for b, line in moved(raw_w[...], hot, block_of):
        ws[0, b] = jnp.where(three, line, 0.0)
        ws[1, b] = jnp.where(three, pltpu.roll(line, SUB - 3, 0), 0.0)
        half_m[b] = jnp.where(three, (0.5 * DT) * jnp.broadcast_to(line[6:7, :], (SUB, BLK)), 0.0)

    slot_lane = lax.broadcasted_iota(I32, (1, slots), 1)
    live = slot_lane < count_s[0]
    owner = jnp.where(live, own_row[...], nb).astype(F32)
    first = lax.broadcasted_iota(I32, (slots, slots), 0)
    second = lax.broadcasted_iota(I32, (slots, slots), 1)
    square = jnp.broadcast_to(owner, (slots, slots))
    unit = jnp.where(first == second, 1.0, 0.0).astype(BF16)
    turned = lax.dot_general(unit, square.astype(BF16), (((1,), (1,)), ((), ())), preferred_element_type=F32)
    ahead = jnp.where((turned == square) & (first < second), 1.0, 0.0)
    earlier = jnp.sum(ahead, axis=0, keepdims=True)
    rank = earlier + jnp.sum(jnp.where(turned < square, 1.0, 0.0), axis=0, keepdims=True)
    chosen_slot = jnp.where(jnp.broadcast_to(rank, (slots, slots)) == first.astype(F32), 1.0, 0.0).astype(BF16)
    list_line = lax.broadcasted_iota(I32, (SUB, slots), 0)
    lists = jnp.where(
        list_line == 0,
        jnp.where(owner < nb, owner, 0.0),
        jnp.where(list_line == 1, other_row[...].astype(F32), jnp.where(earlier > 0.0, 1.0, 0.0)),
    )
    ordered = lax.dot_general(lists.astype(BF16), chosen_slot, (((1,), (1,)), ((), ())), preferred_element_type=F32)
    upto = jnp.sum(jnp.where(turned <= second.astype(F32), 1.0, 0.0), axis=0, keepdims=True)
    some = jnp.sum(jnp.where(turned == second.astype(F32), 1.0, 0.0), axis=0, keepdims=True)
    table_f[...] = jnp.zeros(table_f.shape, F32)
    table_i[...] = jnp.zeros(table_i.shape, I32)
    table_f[:, 0:slots] = ordered
    table_i[:, 0:slots] = jnp.where(list_line == 2, jnp.where(some > 0.0, upto, 0.0), ordered).astype(I32)
    list_copies = [
        pltpu.make_async_copy(table_i, list_s, list_sem.at[0]),
        pltpu.make_async_copy(table_f, keep_s, list_sem.at[1]),
    ]
    for copy in list_copies:
        copy.start()

    for copy in aux_copies:
        copy.wait()
    take_row = jnp.full((SUB, BLK), arow_s[0, 0].astype(F32)) > 0.5
    take_col = jnp.full((SUB, BLK), acol_s[0, 0].astype(F32)) > 0.5
    take_far = jnp.broadcast_to(got_aux[1, 2:3, :], (SUB, BLK)) > 0.5

    def chosen(mine, by_row, by_col, by_both):
        far = jnp.where(take_far, by_both, by_col)
        close = jnp.where(take_row, by_row, mine)
        return jnp.where(take_col, far, close)

    centre = chosen(aux[...], got_aux[0], got_aux[1], got_aux[2])
    centres = [centre[0:1, :], centre[1:2, :]]

    def take_window(source, got):
        for c in range(3):
            for b in range(0, nb, SUB):
                raw[pl.ds(b * SUB + c, SUB, stride=SUB), :] = chosen(
                    source[c, b : b + SUB], got[0, c, b : b + SUB], got[1, c, b : b + SUB], got[2, c, b : b + SUB]
                )

    for copy in x_copies:
        copy.wait()
    take_window(pos, got_x)
    for b, line in moved(raw[...], hot, block_of):
        xs[b] = line

    def take_velocities():
        for copy in list_copies:
            copy.wait()
        for copy in v_copies:
            copy.wait()
        take_window(vel, got_v)
        for b, line in moved(raw[...], hot, block_of):
            vs[b] = line

    def invert():
        block_line = lax.broadcasted_iota(I32, (nb, BLK), 0)
        place = lax.broadcasted_iota(I32, (nb, BLK), 1).astype(F32)
        tops, lows = [], []
        for b in range(nb):
            here = block_of[b : b + 1, :] == block_line
            tops.append(jnp.where(here, float(b), 0.0).astype(BF16))
            lows.append(jnp.where(here, place, 0.0).astype(BF16))
        both = jnp.concatenate([jnp.concatenate(tops, axis=1), jnp.concatenate(lows, axis=1)], axis=0)
        found = lax.dot_general(both, hot[...], (((1,), (1,)), ((), ())), preferred_element_type=F32).astype(I32)
        block_back[...] = found[0:nb]
        spread(found[nb : 2 * nb], hot_back)

    def force(e, meanwhile):
        near = nears[e]
        sums = [jnp.zeros((SUB, BLK), F32), jnp.zeros((SUB, BLK), F32)]
        for b in range(nb):
            x = xs[b]
            near[1, b] = x * SCALE
            for k in range(2):
                sums[k] = sums[k] + ws[k, b] * x
        parts[e, me] = sums[0] + pltpu.roll(sums[1], 3, 0)
        part_copies = []
        for at, target in enumerate(others):
            copy = pltpu.make_async_remote_copy(
                src_ref=parts.at[e, me],
                dst_ref=parts.at[e, me],
                send_sem=part_send.at[e, at],
                recv_sem=part_recv.at[e, at],
                device_id=target,
                device_id_type=MESH,
            )
            copy.start()
            part_copies.append(copy)
        up = pltpu.make_async_remote_copy(
            src_ref=near.at[1, :, 0:3, :],
            dst_ref=near.at[0, :, 0:3, :],
            send_sem=halo_send.at[e, 0],
            recv_sem=halo_recv.at[e, 0],
            device_id=(row, col, lax.rem(me + 1, doms)),
            device_id_type=MESH,
        )
        down = pltpu.make_async_remote_copy(
            src_ref=near.at[1, :, 0:3, :],
            dst_ref=near.at[2, :, 0:3, :],
            send_sem=halo_send.at[e, 1],
            recv_sem=halo_recv.at[e, 1],
            device_id=(row, col, lax.rem(me + doms - 1, doms)),
            device_id_type=MESH,
        )

        @pl.when(me < doms - 1)
        def _():
            up.start()

        @pl.when(me > 0)
        def _():
            down.start()

        def features(slab, b):
            value = near[slab, b]
            high = value.astype(BF16).astype(F32)
            middle = (value - high).astype(BF16).astype(F32)
            kept = high + middle
            square = jnp.where(three, kept * kept, 0.0)
            norm = jnp.broadcast_to(-0.5 * jnp.sum(square, axis=0, keepdims=True), (SUB, BLK))
            one = norm.astype(BF16).astype(F32)
            two = (norm - one).astype(BF16).astype(F32)
            norms = jnp.where(lines == 3, one, jnp.where(lines == 4, two, jnp.where(lines == 5, norm - one - two, 0.0)))
            units = jnp.where((lines >= 3) & (lines < 6), 1.0, 0.0)
            counted = jnp.where(lines == 6, 1.0, 0.0)
            plain = jnp.where(three, high, 0.0)
            fine = jnp.where(three, middle, 0.0)
            theirs = jnp.concatenate([plain + norms + counted, fine + units, plain, fine], axis=0)
            lines_of[slab * nb + b] = theirs[0 : 2 * SUB, :].astype(BF16)
            turned_of[slab * nb + b] = jnp.transpose(theirs).astype(BF16)
            return kept, plain + units, plain + norms, fine

        for b in range(nb):
            kept, top, second_top, fine = features(1, b)
            held[b] = kept
            own_of[b] = jnp.concatenate([top, second_top, fine, fine], axis=0).astype(BF16)

        meanwhile()

        @pl.when(me < doms - 1)
        def _():
            up.wait_send()
            down.wait_recv()

        @pl.when(me > 0)
        def _():
            down.wait_send()
            up.wait_recv()

        for b in range(nb):
            features(0, b)
            features(2, b)

        def ours(p):
            return jnp.clip(list_s[0, p], 0, nb - 1)

        def their(p):
            return jnp.clip(list_s[1, p], 0, 3 * nb - 1)

        def first_of(p):
            return jnp.dot(turned_of[their(p)], own_of[ours(p)], preferred_element_type=F32)

        def second_of(p, carried, logits):
            pieces = [split2(jnp.exp2(logit)) for logit in logits]
            lines_at = [lines_of[their(p + u)] for u in range(2)]
            pulled = jnp.dot(
                jnp.concatenate([jnp.concatenate([line, line], axis=1) for line in lines_at], axis=0),
                jnp.concatenate([jnp.concatenate([pieces[0][h], pieces[1][h]], axis=1) for h in range(2)], axis=0),
                preferred_element_type=F32,
            )
            for u in range(2):
                at = slice(u * BLK, (u + 1) * BLK)
                tile = pulled[2 * u * SUB : (2 * u + 1) * SUB, at] + pulled[(2 * u + 1) * SUB : (2 * u + 2) * SUB, at]
                carried = carried * keep_s[2, p + u] + tile
                prefix[p + u + 1] = carried
            return carried

        def body(i, carried):
            start = i * UNROLL
            ready = [first_of(start + u) for u in range(GROUP)]
            for g in range(0, UNROLL, GROUP):
                later = [first_of(start + g + GROUP + u) for u in range(GROUP)] if g + GROUP < UNROLL else []
                for u in range(0, GROUP, 2):
                    carried = second_of(start + g + u, carried, ready[u : u + 2])
                ready = later
            return carried

        prefix[0] = jnp.zeros((SUB, BLK), F32)
        lax.fori_loop(0, slots // UNROLL, body, jnp.zeros((SUB, BLK), F32))

        for copy in part_copies:
            copy.wait()
        total = parts[e, 0]
        for d in range(1, doms):
            total = total + parts[e, d]
        pulls = []
        for k in range(2):
            collective = jnp.sum(total[3 * k : 3 * k + 3, :], axis=(0, 1), keepdims=True)
            pulls.append(stiff_s[k] * (collective - centres[k]))
        for b in range(nb):
            pulled = prefix[jnp.clip(list_s[2, b], 0, slots)]
            pair = held[b] * jnp.broadcast_to(pulled[6:7, :], (SUB, BLK)) - pulled
            fs[b] = (PAIR_EPS / SCALE) * pair - pulls[0] * ws[0, b] - pulls[1] * ws[1, b]

    force(0, take_velocities)
    for step in range(STEPS):
        for b in range(nb):
            v = vs[b] + half_m[b] * fs[b]
            vs[b] = v
            xs[b] = xs[b] + DT * v
        if step < STEPS - 1:
            force(step + 1, invert if step == 0 else lambda: None)
            for b in range(nb):
                vs[b] = vs[b] + half_m[b] * fs[b]

    def write(source, target):
        for b, line in moved(source[...].reshape(rows, BLK), hot_back, block_back):
            raw[b * SUB : (b + 1) * SUB, :] = line
        for c in range(3):
            target[c] = raw[pl.ds(c, nb, stride=SUB), :]

    def write_state():
        write(xs, out_x)
        write(vs, out_v)

    force(STEPS, write_state)
    write(fs, out_f)
    for c in range(3):
        out_v[c] = out_v[c] + (0.5 * DT) * mass[...] * out_f[c]


def per_device(
    positions, velocities, inv_mass, cv_weight, stiffness, centers, block_order, pair_count, pair_own, pair_other,
    accept_row, accept_col,
):
    atoms = block_order.shape[0]
    nb = atoms // BLK
    slots = pair_own.shape[1]
    doms = lax.axis_size("dom")
    evals = STEPS + 1
    wide = BLK * pl.cdiv(slots, BLK)
    vmem = pl.BlockSpec(memory_space=pltpu.VMEM)
    smem = pl.BlockSpec(memory_space=pltpu.SMEM)
    dma = pltpu.SemaphoreType.DMA
    shape = jax.ShapeDtypeStruct((3, nb, BLK), F32)
    state = pltpu.VMEM((nb, SUB, BLK), F32)
    weights = cv_weight.transpose(1, 0, 2).reshape(3, 2, nb, BLK).transpose(0, 2, 1, 3).reshape(6 * nb, BLK)
    outs = pl.pallas_call(
        functools.partial(kernel, (doms, nb, slots)),
        out_shape=(shape, shape, shape),
        in_specs=[vmem] * 7 + [smem] * 5,
        out_specs=(vmem, vmem, vmem),
        scratch_shapes=[
            pltpu.VMEM((BLK, atoms), BF16),
            pltpu.VMEM((BLK, atoms), BF16),
            pltpu.VMEM((nb, BLK), I32),
            pltpu.VMEM((nb, BLK), I32),
            pltpu.VMEM((nb * SUB, BLK), F32),
            pltpu.VMEM((nb * SUB, BLK), F32),
            pltpu.VMEM((3, 3, nb, BLK), F32),
            pltpu.VMEM((3, 3, nb, BLK), F32),
            pltpu.VMEM((3, SUB, BLK), F32),
            pltpu.VMEM((SUB, BLK), F32),
            pltpu.VMEM((evals, doms, SUB, BLK), F32),
            pltpu.VMEM((slots + 1, SUB, BLK), F32),
            pltpu.VMEM((3 * nb, 2 * SUB, BLK), BF16),
            pltpu.VMEM((3 * nb, BLK, 4 * SUB), BF16),
            pltpu.VMEM((nb, 4 * SUB, BLK), BF16),
            pltpu.VMEM((SUB, wide), I32),
            pltpu.VMEM((SUB, wide), F32),
            pltpu.SMEM((SUB, wide), I32),
            pltpu.SMEM((SUB, wide), F32),
            state, state, state, state, state,
            pltpu.VMEM((2, nb, SUB, BLK), F32),
            dma((3,)), dma((3,)), dma((3,)), dma((3,)), dma((3,)), dma((3,)),
            dma((evals, 2)), dma((evals, 2)), dma((evals, doms)), dma((evals, doms)), dma((2,)),
        ]
        + [pltpu.VMEM((3, nb, SUB, BLK), F32)] * evals,
        compiler_params=pltpu.CompilerParams(collective_id=0, has_side_effects=True),
        name="windows",
    )(
        positions.reshape(3, nb, BLK), velocities.reshape(3, nb, BLK), inv_mass.reshape(nb, BLK), weights, block_order.reshape(nb, BLK), pair_own,
        pair_other, pair_count, stiffness, centers[0], accept_row, accept_col,
    )
    return tuple(out.reshape(1, 1, 3, atoms) for out in outs)


def solution(mesh):
    placed = (
        P("wrow", "wcol", None, "dom"),
        P("wrow", "wcol", None, "dom"),
        P("dom"),
        P(None, None, "dom"),
        P(),
        P("wrow", "wcol", None),
        P("dom"),
        P("dom"),
        P("dom", None),
        P("dom", None),
        P("wrow", "wcol"),
        P("wrow", "wcol"),
    )
    return jax.shard_map(
        per_device,
        mesh=mesh,
        in_specs=placed,
        out_specs=(
            P("wrow", "wcol", None, "dom"),
            P("wrow", "wcol", None, "dom"),
            P("wrow", "wcol", None, "dom"),
        ),
        check_vma=False,
    )
```

```python
import functools
import math

import jax
import jax.numpy as jnp
from jax import lax
from jax.experimental import pallas as pl
from jax.experimental.pallas import tpu as pltpu
from jax.sharding import PartitionSpec as P

BLK = 128
SUB = 8
STEPS = 3
PAIR_EPS = 0.015625
DT = 0.1
SCALE = math.sqrt(math.log2(math.e))
GROUP = 8
UNROLL = 64
MESH = pl.DeviceIdType.MESH
F32 = jnp.float32
BF16 = jnp.bfloat16
I32 = jnp.int32


def split2(value):
    high = value.astype(BF16)
    return high, (value - high.astype(F32)).astype(BF16)


def kernel(
    sizes,
    pos, vel, mass, cvw, order, own_row, other_row, count_s, stiff_s, centers_s, arow_s, acol_s,
    out_x, out_v, out_f,
    hot, hot_back, block_of, block_back, raw, raw_w, got_x, got_v, got_aux, aux, parts, prefix, lines_of, turned_of, own_of,
    table_i, table_f, list_s, keep_s, xs, vs, fs, held, half_m, ws, near_w, cross_parts, cross_last,
    sx_send, sx_recv, sv_send, sv_recv, sa_send, sa_recv, halo_send, halo_recv, part_send, part_recv, list_sem, weight_send, weight_recv, cross_send, cross_recv, *nears,
):
    doms, nb, slots = sizes
    rows = nb * SUB
    row = lax.axis_index("wrow")
    col = lax.axis_index("wcol")
    me = lax.axis_index("dom")
    row_to = row + 1 - 2 * lax.rem(row, 2)
    col_to = col + 1 - 2 * lax.rem(col, 2)
    partners = [(row_to, col, me), (row, col_to, me), (row_to, col_to, me)]
    others = [(row, col, lax.rem(me + off, doms)) for off in range(1, doms)]

    lines = lax.broadcasted_iota(I32, (SUB, BLK), 0)
    aux[...] = jnp.where(
        lines == 0,
        centers_s[0, 0],
        jnp.where(lines == 1, centers_s[0, 1], arow_s[0, 0].astype(F32)),
    )
    barrier = pltpu.get_barrier_semaphore()
    for target in partners + others:
        pl.semaphore_signal(barrier, inc=1, device_id=target, device_id_type=MESH)
    pl.semaphore_wait(barrier, len(partners) + len(others))

    def exchange(source, target, sends, recvs):
        copies = []
        for at, partner in enumerate(partners):
            copy = pltpu.make_async_remote_copy(
                src_ref=source,
                dst_ref=target.at[at],
                send_sem=sends.at[at],
                recv_sem=recvs.at[at],
                device_id=partner,
                device_id_type=MESH,
            )
            copy.start()
            copies.append(copy)
        return copies

    aux_copies = exchange(aux, got_aux, sa_send, sa_recv)
    x_copies = exchange(pos, got_x, sx_send, sx_recv)
    v_copies = exchange(vel, got_v, sv_send, sv_recv)

    lane_line = lax.broadcasted_iota(I32, (BLK, BLK), 0)

    def spread(low, target):
        for b in range(nb):
            target[:, b * BLK : (b + 1) * BLK] = jnp.where(low[b : b + 1, :] == lane_line, 1.0, 0.0).astype(BF16)

    listed = order[...]
    block_of[...] = lax.div(listed, BLK)
    spread(lax.rem(listed, BLK), hot)

    def moved(source, hots, blocks):
        left = jnp.concatenate(split2(source), axis=1)
        for b in range(0, nb, 2):
            right = hots[:, b * BLK : (b + 2) * BLK]
            got = jnp.dot(left, jnp.concatenate([right, right], axis=0), preferred_element_type=F32)
            for u in range(2):
                home = jnp.broadcast_to(blocks[b + u : b + u + 1, :], (SUB, BLK))
                line = got[0:SUB, u * BLK : (u + 1) * BLK]
                for s in range(1, nb):
                    line = jnp.where(home == s, got[s * SUB : (s + 1) * SUB, u * BLK : (u + 1) * BLK], line)
                yield b + u, line

    raw[...] = jnp.zeros((rows, BLK), F32)
    raw_w[...] = jnp.zeros((rows, BLK), F32)
    for k in range(2):
        for c in range(3):
            raw_w[pl.ds(3 * k + c, nb, stride=SUB), :] = cvw[pl.ds(2 * nb * c + k, nb, stride=2), :]
    raw_w[pl.ds(6, nb, stride=SUB), :] = mass[...]
    three = lines < 3
    for b, line in moved(raw_w[...], hot, block_of):
        ws[0, b] = jnp.where(three, line, 0.0)
        ws[1, b] = jnp.where(three, pltpu.roll(line, SUB - 3, 0), 0.0)
        half_m[b] = jnp.where(three, (0.5 * DT) * jnp.broadcast_to(line[6:7, :], (SUB, BLK)), 0.0)
    cross = [jnp.zeros((SUB, BLK), F32) for _ in range(3)]
    for b in range(nb):
        for k in range(2):
            shift = DT * half_m[b] * ws[k, b]
            near_w[1, k, b] = shift
            for j in range(k, 2):
                cross[k + j] = cross[k + j] + shift * ws[j, b]
    cross_parts[me] = cross[0] + pltpu.roll(cross[1], 3, 0)
    cross_last[me] = cross[2]
    early = []
    for at, target in enumerate(others):
        for which, held_parts in enumerate((cross_parts, cross_last)):
            copy = pltpu.make_async_remote_copy(
                src_ref=held_parts.at[me],
                dst_ref=held_parts.at[me],
                send_sem=cross_send.at[which, at],
                recv_sem=cross_recv.at[which, at],
                device_id=target,
                device_id_type=MESH,
            )
            copy.start()
            early.append(copy)

    def neighbours(ref, sends, recvs):
        source = ref.at[1, ..., 0:3, :]
        return tuple(
            pltpu.make_async_remote_copy(
                src_ref=source,
                dst_ref=ref.at[1 - step, ..., 0:3, :],
                send_sem=sends.at[at],
                recv_sem=recvs.at[at],
                device_id=(row, col, lax.rem(me + doms + step, doms)),
                device_id_type=MESH,
            )
            for at, step in enumerate((1, -1))
        )

    def send_both(up, down):
        @pl.when(me < doms - 1)
        def _():
            up.start()

        @pl.when(me > 0)
        def _():
            down.start()

    def wait_both(up, down):
        @pl.when(me < doms - 1)
        def _():
            up.wait_send()
            down.wait_recv()

        @pl.when(me > 0)
        def _():
            down.wait_send()
            up.wait_recv()

    weight_halo = neighbours(near_w, weight_send, weight_recv)
    send_both(*weight_halo)

    slot_lane = lax.broadcasted_iota(I32, (1, slots), 1)
    live = slot_lane < count_s[0]
    owner = jnp.where(live, own_row[...], nb).astype(F32)
    first = lax.broadcasted_iota(I32, (slots, slots), 0)
    second = lax.broadcasted_iota(I32, (slots, slots), 1)
    square = jnp.broadcast_to(owner, (slots, slots))
    unit = jnp.where(first == second, 1.0, 0.0).astype(BF16)
    turned = lax.dot_general(unit, square.astype(BF16), (((1,), (1,)), ((), ())), preferred_element_type=F32)
    ahead = jnp.where((turned == square) & (first < second), 1.0, 0.0)
    earlier = jnp.sum(ahead, axis=0, keepdims=True)
    rank = earlier + jnp.sum(jnp.where(turned < square, 1.0, 0.0), axis=0, keepdims=True)
    chosen_slot = jnp.where(jnp.broadcast_to(rank, (slots, slots)) == first.astype(F32), 1.0, 0.0).astype(BF16)
    list_line = lax.broadcasted_iota(I32, (SUB, slots), 0)
    lists = jnp.where(
        list_line == 0,
        jnp.where(owner < nb, owner, 0.0),
        jnp.where(list_line == 1, other_row[...].astype(F32), jnp.where(earlier > 0.0, 1.0, 0.0)),
    )
    ordered = lax.dot_general(lists.astype(BF16), chosen_slot, (((1,), (1,)), ((), ())), preferred_element_type=F32)
    upto = jnp.sum(jnp.where(turned <= second.astype(F32), 1.0, 0.0), axis=0, keepdims=True)
    some = jnp.sum(jnp.where(turned == second.astype(F32), 1.0, 0.0), axis=0, keepdims=True)
    table_f[...] = jnp.zeros(table_f.shape, F32)
    table_i[...] = jnp.zeros(table_i.shape, I32)
    table_f[:, 0:slots] = ordered
    table_i[:, 0:slots] = jnp.where(list_line == 2, jnp.where(some > 0.0, upto, 0.0), ordered).astype(I32)
    list_copies = [
        pltpu.make_async_copy(table_i, list_s, list_sem.at[0]),
        pltpu.make_async_copy(table_f, keep_s, list_sem.at[1]),
    ]
    for copy in list_copies:
        copy.start()

    for copy in aux_copies:
        copy.wait()
    take_row = jnp.full((SUB, BLK), arow_s[0, 0].astype(F32)) > 0.5
    take_col = jnp.full((SUB, BLK), acol_s[0, 0].astype(F32)) > 0.5
    take_far = jnp.broadcast_to(got_aux[1, 2:3, :], (SUB, BLK)) > 0.5

    def chosen(mine, by_row, by_col, by_both):
        far = jnp.where(take_far, by_both, by_col)
        close = jnp.where(take_row, by_row, mine)
        return jnp.where(take_col, far, close)

    centre = chosen(aux[...], got_aux[0], got_aux[1], got_aux[2])
    centres = [centre[0:1, :], centre[1:2, :]]

    def take_window(source, got):
        for c in range(3):
            for b in range(0, nb, SUB):
                raw[pl.ds(b * SUB + c, SUB, stride=SUB), :] = chosen(
                    source[c, b : b + SUB], got[0, c, b : b + SUB], got[1, c, b : b + SUB], got[2, c, b : b + SUB]
                )

    for copy in x_copies:
        copy.wait()
    take_window(pos, got_x)
    for b, line in moved(raw[...], hot, block_of):
        xs[b] = line

    def take_velocities():
        for copy in list_copies:
            copy.wait()
        for copy in v_copies:
            copy.wait()
        take_window(vel, got_v)
        for b, line in moved(raw[...], hot, block_of):
            vs[b] = line

    def invert():
        block_line = lax.broadcasted_iota(I32, (nb, BLK), 0)
        place = lax.broadcasted_iota(I32, (nb, BLK), 1).astype(F32)
        tops, lows = [], []
        for b in range(nb):
            here = block_of[b : b + 1, :] == block_line
            tops.append(jnp.where(here, float(b), 0.0).astype(BF16))
            lows.append(jnp.where(here, place, 0.0).astype(BF16))
        both = jnp.concatenate([jnp.concatenate(tops, axis=1), jnp.concatenate(lows, axis=1)], axis=0)
        found = lax.dot_general(both, hot[...], (((1,), (1,)), ((), ())), preferred_element_type=F32).astype(I32)
        block_back[...] = found[0:nb]
        spread(found[nb : 2 * nb], hot_back)

    def launch(e):
        near = nears[e]
        sums = [jnp.zeros((SUB, BLK), F32), jnp.zeros((SUB, BLK), F32)]
        for b in range(nb):
            x = xs[b]
            near[1, b] = x
            for k in range(2):
                sums[k] = sums[k] + ws[k, b] * x
        parts[e, me] = sums[0] + pltpu.roll(sums[1], 3, 0)
        part_copies = []
        for at, target in enumerate(others):
            copy = pltpu.make_async_remote_copy(
                src_ref=parts.at[e, me],
                dst_ref=parts.at[e, me],
                send_sem=part_send.at[e, at],
                recv_sem=part_recv.at[e, at],
                device_id=target,
                device_id_type=MESH,
            )
            copy.start()
            part_copies.append(copy)
        halo = neighbours(near, halo_send.at[e], halo_recv.at[e])
        send_both(*halo)
        return part_copies, halo

    def whole(tile, first):
        return jnp.sum(tile[first : first + 3, :], axis=(0, 1), keepdims=True)

    def settle(e, part_copies, before, crossed):
        for copy in part_copies:
            copy.wait()
        total = parts[e, 0]
        for d in range(1, doms):
            total = total + parts[e, d]
        pulls = []
        for k in range(2):
            collective = whole(total, 3 * k)
            if before is not None:
                collective = collective - before[0] * crossed[k] - before[1] * crossed[k + 1]
            pulls.append(stiff_s[k] * (collective - centres[k][:, 0:1]))
        return pulls

    def pairs(e, halo, before, meanwhile):
        near = nears[e]

        def features(slab, b, value):
            value = value * SCALE
            high = value.astype(BF16).astype(F32)
            middle = (value - high).astype(BF16).astype(F32)
            kept = high + middle
            square = jnp.where(three, kept * kept, 0.0)
            norm = jnp.broadcast_to(-0.5 * jnp.sum(square, axis=0, keepdims=True), (SUB, BLK))
            one = norm.astype(BF16).astype(F32)
            two = (norm - one).astype(BF16).astype(F32)
            norms = jnp.where(lines == 3, one, jnp.where(lines == 4, two, jnp.where(lines == 5, norm - one - two, 0.0)))
            units = jnp.where((lines >= 3) & (lines < 6), 1.0, 0.0)
            counted = jnp.where(lines == 6, 1.0, 0.0)
            plain = jnp.where(three, high, 0.0)
            fine = jnp.where(three, middle, 0.0)
            theirs = jnp.concatenate([plain + norms + counted, fine + units, plain, fine], axis=0)
            lines_of[slab * nb + b] = theirs[0 : 2 * SUB, :].astype(BF16)
            turned_of[slab * nb + b] = jnp.transpose(theirs).astype(BF16)
            return kept, plain + units, plain + norms, fine

        for b in range(nb):
            kept, top, second_top, fine = features(1, b, xs[b])
            held[b] = kept
            own_of[b] = jnp.concatenate([top, second_top, fine, fine], axis=0).astype(BF16)

        meanwhile()

        wait_both(*halo)
        for b in range(nb):
            for slab in (0, 2):
                value = near[slab, b]
                if before is not None:
                    value = value - before[0] * near_w[slab, 0, b] - before[1] * near_w[slab, 1, b]
                features(slab, b, value)

        def ours(p):
            return jnp.clip(list_s[0, p], 0, nb - 1)

        def their(p):
            return jnp.clip(list_s[1, p], 0, 3 * nb - 1)

        def first_of(p):
            return jnp.dot(turned_of[their(p)], own_of[ours(p)], preferred_element_type=F32)

        def second_of(p, carried, logits):
            pieces = [split2(jnp.exp2(logit)) for logit in logits]
            lines_at = [lines_of[their(p + u)] for u in range(2)]
            pulled = jnp.dot(
                jnp.concatenate([jnp.concatenate([line, line], axis=1) for line in lines_at], axis=0),
                jnp.concatenate([jnp.concatenate([pieces[0][h], pieces[1][h]], axis=1) for h in range(2)], axis=0),
                preferred_element_type=F32,
            )
            for u in range(2):
                at = slice(u * BLK, (u + 1) * BLK)
                tile = pulled[2 * u * SUB : (2 * u + 1) * SUB, at] + pulled[(2 * u + 1) * SUB : (2 * u + 2) * SUB, at]
                carried = carried * keep_s[2, p + u] + tile
                prefix[p + u + 1] = carried
            return carried

        def body(i, carried):
            start = i * UNROLL
            ready = [first_of(start + u) for u in range(GROUP)]
            for g in range(0, UNROLL, GROUP):
                later = [first_of(start + g + GROUP + u) for u in range(GROUP)] if g + GROUP < UNROLL else []
                for u in range(0, GROUP, 2):
                    carried = second_of(start + g + u, carried, ready[u : u + 2])
                ready = later
            return carried

        prefix[0] = jnp.zeros((SUB, BLK), F32)
        lax.fori_loop(0, slots // UNROLL, body, jnp.zeros((SUB, BLK), F32))

    def write(source, target):
        for b, line in moved(source[...].reshape(rows, BLK), hot_back, block_back):
            raw[b * SUB : (b + 1) * SUB, :] = line
        for c in range(3):
            target[c] = raw[pl.ds(c, nb, stride=SUB), :]

    def write_state():
        write(xs, out_x)
        write(vs, out_v)

    def pair_force(b):
        pulled = prefix[jnp.clip(list_s[2, b], 0, slots)]
        return (PAIR_EPS / SCALE) * (held[b] * jnp.broadcast_to(pulled[6:7, :], (SUB, BLK)) - pulled)

    part_copies, halo = launch(0)
    pairs(0, halo, None, take_velocities)
    before = crossed = None
    for step in range(STEPS):
        kick = 1.0 if step == 0 else 2.0
        for b in range(nb):
            pair = pair_force(b)
            fs[b] = pair
            xs[b] = xs[b] + DT * (vs[b] + kick * half_m[b] * pair)
        next_copies, halo = launch(step + 1)
        pulls = settle(step, part_copies, before, crossed)
        before = [jnp.broadcast_to(kick * pull, (SUB, BLK)) for pull in pulls]
        for b in range(nb):
            vs[b] = vs[b] + kick * half_m[b] * (fs[b] - pulls[0] * ws[0, b] - pulls[1] * ws[1, b])
            xs[b] = xs[b] - before[0] * near_w[1, 0, b] - before[1] * near_w[1, 1, b]
        before_sum = [kick * pull for pull in pulls]

        def meanwhile():
            if step == 0:
                wait_both(*weight_halo)
                invert()
            if step == STEPS - 1:
                write_state()

        if step == 0:
            for copy in early:
                copy.wait()
            total = cross_parts[0]
            last = cross_last[0]
            for d in range(1, doms):
                total = total + cross_parts[d]
                last = last + cross_last[d]
            crossed = [whole(total, 0), whole(total, 3), whole(last, 0)]
        pairs(step + 1, halo, before, meanwhile)
        before = before_sum
        part_copies = next_copies
    pulls = settle(STEPS, part_copies, before, crossed)
    for b in range(nb):
        fs[b] = pair_force(b) - pulls[0] * ws[0, b] - pulls[1] * ws[1, b]
    write(fs, out_f)


def finish(mass, x, v, f, out_x, out_v, out_f):
    out_x[...] = x[...]
    out_f[...] = f[...]
    out_v[...] = v[...] + (0.5 * DT) * mass[...][None] * f[...]


def per_device(
    positions, velocities, inv_mass, cv_weight, stiffness, centers, block_order, pair_count, pair_own, pair_other,
    accept_row, accept_col,
):
    atoms = block_order.shape[0]
    nb = atoms // BLK
    slots = pair_own.shape[1]
    doms = lax.axis_size("dom")
    evals = STEPS + 1
    wide = BLK * pl.cdiv(slots, BLK)
    vmem = pl.BlockSpec(memory_space=pltpu.VMEM)
    smem = pl.BlockSpec(memory_space=pltpu.SMEM)
    dma = pltpu.SemaphoreType.DMA
    shape = jax.ShapeDtypeStruct((3, nb, BLK), F32)
    state = pltpu.VMEM((nb, SUB, BLK), F32)
    weights = cv_weight.transpose(1, 0, 2).reshape(3, 2, nb, BLK).transpose(0, 2, 1, 3).reshape(6 * nb, BLK)
    outs = pl.pallas_call(
        functools.partial(kernel, (doms, nb, slots)),
        out_shape=(shape, shape, shape),
        in_specs=[vmem] * 7 + [smem] * 5,
        out_specs=(vmem, vmem, vmem),
        scratch_shapes=[
            pltpu.VMEM((BLK, atoms), BF16),
            pltpu.VMEM((BLK, atoms), BF16),
            pltpu.VMEM((nb, BLK), I32),
            pltpu.VMEM((nb, BLK), I32),
            pltpu.VMEM((nb * SUB, BLK), F32),
            pltpu.VMEM((nb * SUB, BLK), F32),
            pltpu.VMEM((3, 3, nb, BLK), F32),
            pltpu.VMEM((3, 3, nb, BLK), F32),
            pltpu.VMEM((3, SUB, BLK), F32),
            pltpu.VMEM((SUB, BLK), F32),
            pltpu.VMEM((evals, doms, SUB, BLK), F32),
            pltpu.VMEM((slots + 1, SUB, BLK), F32),
            pltpu.VMEM((3 * nb, 2 * SUB, BLK), BF16),
            pltpu.VMEM((3 * nb, BLK, 4 * SUB), BF16),
            pltpu.VMEM((nb, 4 * SUB, BLK), BF16),
            pltpu.VMEM((SUB, wide), I32),
            pltpu.VMEM((SUB, wide), F32),
            pltpu.SMEM((SUB, wide), I32),
            pltpu.SMEM((SUB, wide), F32),
            state, state, state, state, state,
            pltpu.VMEM((2, nb, SUB, BLK), F32),
            pltpu.VMEM((3, 2, nb, SUB, BLK), F32),
            pltpu.VMEM((doms, SUB, BLK), F32),
            pltpu.VMEM((doms, SUB, BLK), F32),
            dma((3,)), dma((3,)), dma((3,)), dma((3,)), dma((3,)), dma((3,)),
            dma((evals, 2)), dma((evals, 2)), dma((evals, doms)), dma((evals, doms)), dma((2,)),
            dma((2,)), dma((2,)), dma((2, doms)), dma((2, doms)),
        ]
        + [pltpu.VMEM((3, nb, SUB, BLK), F32)] * evals,
        compiler_params=pltpu.CompilerParams(collective_id=0, has_side_effects=True),
        name="windows",
    )(
        positions.reshape(3, nb, BLK), velocities.reshape(3, nb, BLK), inv_mass.reshape(nb, BLK), weights, block_order.reshape(nb, BLK), pair_own,
        pair_other, pair_count, stiffness, centers[0], accept_row, accept_col,
    )
    outs = pl.pallas_call(
        finish,
        out_shape=(shape, shape, shape),
        in_specs=[vmem] * 4,
        out_specs=(vmem, vmem, vmem),
        name="finish",
    )(inv_mass.reshape(nb, BLK), *outs)
    return tuple(out.reshape(1, 1, 3, atoms) for out in outs)


def solution(mesh):
    placed = (
        P("wrow", "wcol", None, "dom"),
        P("wrow", "wcol", None, "dom"),
        P("dom"),
        P(None, None, "dom"),
        P(),
        P("wrow", "wcol", None),
        P("dom"),
        P("dom"),
        P("dom", None),
        P("dom", None),
        P("wrow", "wcol"),
        P("wrow", "wcol"),
    )
    return jax.shard_map(
        per_device,
        mesh=mesh,
        in_specs=placed,
        out_specs=(
            P("wrow", "wcol", None, "dom"),
            P("wrow", "wcol", None, "dom"),
            P("wrow", "wcol", None, "dom"),
        ),
        check_vma=False,
    )
```

```python
import functools
import math

import jax
import jax.numpy as jnp
from jax import lax
from jax.experimental import pallas as pl
from jax.experimental.pallas import tpu as pltpu
from jax.sharding import PartitionSpec as P

BLK = 128
SUB = 8
STEPS = 3
PAIR_EPS = 0.015625
DT = 0.1
SCALE = math.sqrt(math.log2(math.e))
GROUP = 8
UNROLL = 64
MESH = pl.DeviceIdType.MESH
F32 = jnp.float32
BF16 = jnp.bfloat16
I32 = jnp.int32


def split2(value):
    high = value.astype(BF16)
    return high, (value - high.astype(F32)).astype(BF16)


def kernel(
    sizes,
    pos_h, vel_h, mass_h, cvw_h, order_h, own_h, other_h, count_h, stiff_h, centers_h, arow_h, acol_h,
    out_x, out_v, out_f,
    pos, vel, mass, cvw, order, own_row, other_row, count_s, stiff_s, centers_s, arow_s, acol_s, in_sem,
    hot, hot_back, block_of, block_back, raw, raw_w, got_x, got_v, got_aux, aux, parts, prefix, lines_of, turned_of, own_of,
    table_i, table_f, list_s, keep_s, xs, vs, fs, held, half_m, ws, near_w, cross_parts, cross_last,
    sx_send, sx_recv, sv_send, sv_recv, sa_send, sa_recv, halo_send, halo_recv, part_send, part_recv, list_sem, weight_send, weight_recv, cross_send, cross_recv, *nears,
):
    doms, nb, slots = sizes
    rows = nb * SUB
    row = lax.axis_index("wrow")
    col = lax.axis_index("wcol")
    me = lax.axis_index("dom")
    row_to = row + 1 - 2 * lax.rem(row, 2)
    col_to = col + 1 - 2 * lax.rem(col, 2)
    partners = [(row_to, col, me), (row, col_to, me), (row_to, col_to, me)]
    others = [(row, col, lax.rem(me + off, doms)) for off in range(1, doms)]

    barrier = pltpu.get_barrier_semaphore()
    for target in partners + others:
        pl.semaphore_signal(barrier, inc=1, device_id=target, device_id_type=MESH)
    entered = [
        pltpu.make_async_copy(source, target, in_sem.at[at])
        for at, (source, target) in enumerate((
            (centers_h, centers_s), (arow_h, arow_s), (pos_h, pos), (vel_h, vel), (order_h, order), (cvw_h, cvw), (mass_h, mass),
            (own_h, own_row), (other_h, other_row), (count_h, count_s), (stiff_h, stiff_s), (acol_h, acol_s),
        ))
    ]
    for copy in entered:
        copy.start()
    for copy in entered[0:4]:
        copy.wait()
    lines = lax.broadcasted_iota(I32, (SUB, BLK), 0)
    aux[...] = jnp.where(
        lines == 0,
        centers_s[0, 0],
        jnp.where(lines == 1, centers_s[0, 1], arow_s[0, 0].astype(F32)),
    )
    pl.semaphore_wait(barrier, len(partners) + len(others))

    def exchange(source, target, sends, recvs):
        copies = []
        for at, partner in enumerate(partners):
            copy = pltpu.make_async_remote_copy(
                src_ref=source,
                dst_ref=target.at[at],
                send_sem=sends.at[at],
                recv_sem=recvs.at[at],
                device_id=partner,
                device_id_type=MESH,
            )
            copy.start()
            copies.append(copy)
        return copies

    aux_copies = exchange(aux, got_aux, sa_send, sa_recv)
    x_copies = exchange(pos, got_x, sx_send, sx_recv)
    v_copies = exchange(vel, got_v, sv_send, sv_recv)

    for copy in entered[4:]:
        copy.wait()
    lane_line = lax.broadcasted_iota(I32, (BLK, BLK), 0)

    def spread(low, target):
        for b in range(nb):
            target[:, b * BLK : (b + 1) * BLK] = jnp.where(low[b : b + 1, :] == lane_line, 1.0, 0.0).astype(BF16)

    listed = order[...]
    block_of[...] = lax.div(listed, BLK)
    spread(lax.rem(listed, BLK), hot)

    def moved(source, hots, blocks):
        left = jnp.concatenate(split2(source), axis=1)
        for b in range(0, nb, 2):
            right = hots[:, b * BLK : (b + 2) * BLK]
            got = jnp.dot(left, jnp.concatenate([right, right], axis=0), preferred_element_type=F32)
            for u in range(2):
                home = jnp.broadcast_to(blocks[b + u : b + u + 1, :], (SUB, BLK))
                line = got[0:SUB, u * BLK : (u + 1) * BLK]
                for s in range(1, nb):
                    line = jnp.where(home == s, got[s * SUB : (s + 1) * SUB, u * BLK : (u + 1) * BLK], line)
                yield b + u, line

    raw[...] = jnp.zeros((rows, BLK), F32)
    raw_w[...] = jnp.zeros((rows, BLK), F32)
    for k in range(2):
        for c in range(3):
            raw_w[pl.ds(3 * k + c, nb, stride=SUB), :] = cvw[pl.ds(2 * nb * c + k, nb, stride=2), :]
    raw_w[pl.ds(6, nb, stride=SUB), :] = mass[...]
    three = lines < 3
    for b, line in moved(raw_w[...], hot, block_of):
        ws[0, b] = jnp.where(three, line, 0.0)
        ws[1, b] = jnp.where(three, pltpu.roll(line, SUB - 3, 0), 0.0)
        half_m[b] = jnp.where(three, (0.5 * DT) * jnp.broadcast_to(line[6:7, :], (SUB, BLK)), 0.0)
    cross = [jnp.zeros((SUB, BLK), F32) for _ in range(3)]
    for b in range(nb):
        for k in range(2):
            shift = DT * half_m[b] * ws[k, b]
            near_w[1, k, b] = shift
            for j in range(k, 2):
                cross[k + j] = cross[k + j] + shift * ws[j, b]
    cross_parts[me] = cross[0] + pltpu.roll(cross[1], 3, 0)
    cross_last[me] = cross[2]
    early = []
    for at, target in enumerate(others):
        for which, held_parts in enumerate((cross_parts, cross_last)):
            copy = pltpu.make_async_remote_copy(
                src_ref=held_parts.at[me],
                dst_ref=held_parts.at[me],
                send_sem=cross_send.at[which, at],
                recv_sem=cross_recv.at[which, at],
                device_id=target,
                device_id_type=MESH,
            )
            copy.start()
            early.append(copy)

    def neighbours(ref, sends, recvs):
        source = ref.at[1, ..., 0:3, :]
        return tuple(
            pltpu.make_async_remote_copy(
                src_ref=source,
                dst_ref=ref.at[1 - step, ..., 0:3, :],
                send_sem=sends.at[at],
                recv_sem=recvs.at[at],
                device_id=(row, col, lax.rem(me + doms + step, doms)),
                device_id_type=MESH,
            )
            for at, step in enumerate((1, -1))
        )

    def send_both(up, down):
        @pl.when(me < doms - 1)
        def _():
            up.start()

        @pl.when(me > 0)
        def _():
            down.start()

    def wait_both(up, down):
        @pl.when(me < doms - 1)
        def _():
            up.wait_send()
            down.wait_recv()

        @pl.when(me > 0)
        def _():
            down.wait_send()
            up.wait_recv()

    weight_halo = neighbours(near_w, weight_send, weight_recv)
    send_both(*weight_halo)

    slot_lane = lax.broadcasted_iota(I32, (1, slots), 1)
    live = slot_lane < count_s[0]
    owner = jnp.where(live, own_row[...], nb).astype(F32)
    first = lax.broadcasted_iota(I32, (slots, slots), 0)
    second = lax.broadcasted_iota(I32, (slots, slots), 1)
    square = jnp.broadcast_to(owner, (slots, slots))
    unit = jnp.where(first == second, 1.0, 0.0).astype(BF16)
    turned = lax.dot_general(unit, square.astype(BF16), (((1,), (1,)), ((), ())), preferred_element_type=F32)
    ahead = jnp.where((turned == square) & (first < second), 1.0, 0.0)
    earlier = jnp.sum(ahead, axis=0, keepdims=True)
    rank = earlier + jnp.sum(jnp.where(turned < square, 1.0, 0.0), axis=0, keepdims=True)
    chosen_slot = jnp.where(jnp.broadcast_to(rank, (slots, slots)) == first.astype(F32), 1.0, 0.0).astype(BF16)
    list_line = lax.broadcasted_iota(I32, (SUB, slots), 0)
    lists = jnp.where(
        list_line == 0,
        jnp.where(owner < nb, owner, 0.0),
        jnp.where(list_line == 1, other_row[...].astype(F32), jnp.where(earlier > 0.0, 1.0, 0.0)),
    )
    ordered = lax.dot_general(lists.astype(BF16), chosen_slot, (((1,), (1,)), ((), ())), preferred_element_type=F32)
    upto = jnp.sum(jnp.where(turned <= second.astype(F32), 1.0, 0.0), axis=0, keepdims=True)
    some = jnp.sum(jnp.where(turned == second.astype(F32), 1.0, 0.0), axis=0, keepdims=True)
    table_f[...] = jnp.zeros(table_f.shape, F32)
    table_i[...] = jnp.zeros(table_i.shape, I32)
    table_f[:, 0:slots] = ordered
    table_i[:, 0:slots] = jnp.where(list_line == 2, jnp.where(some > 0.0, upto, 0.0), ordered).astype(I32)
    list_copies = [
        pltpu.make_async_copy(table_i, list_s, list_sem.at[0]),
        pltpu.make_async_copy(table_f, keep_s, list_sem.at[1]),
    ]
    for copy in list_copies:
        copy.start()

    for copy in aux_copies:
        copy.wait()
    take_row = jnp.full((SUB, BLK), arow_s[0, 0].astype(F32)) > 0.5
    take_col = jnp.full((SUB, BLK), acol_s[0, 0].astype(F32)) > 0.5
    take_far = jnp.broadcast_to(got_aux[1, 2:3, :], (SUB, BLK)) > 0.5

    def chosen(mine, by_row, by_col, by_both):
        far = jnp.where(take_far, by_both, by_col)
        close = jnp.where(take_row, by_row, mine)
        return jnp.where(take_col, far, close)

    centre = chosen(aux[...], got_aux[0], got_aux[1], got_aux[2])
    centres = [centre[0:1, :], centre[1:2, :]]

    def take_window(source, got):
        for c in range(3):
            for b in range(0, nb, SUB):
                raw[pl.ds(b * SUB + c, SUB, stride=SUB), :] = chosen(
                    source[c, b : b + SUB], got[0, c, b : b + SUB], got[1, c, b : b + SUB], got[2, c, b : b + SUB]
                )

    for copy in x_copies:
        copy.wait()
    take_window(pos, got_x)
    for b, line in moved(raw[...], hot, block_of):
        xs[b] = line

    def take_velocities():
        for copy in list_copies:
            copy.wait()
        for copy in v_copies:
            copy.wait()
        take_window(vel, got_v)
        for b, line in moved(raw[...], hot, block_of):
            vs[b] = line

    def invert():
        block_line = lax.broadcasted_iota(I32, (nb, BLK), 0)
        place = lax.broadcasted_iota(I32, (nb, BLK), 1).astype(F32)
        tops, lows = [], []
        for b in range(nb):
            here = block_of[b : b + 1, :] == block_line
            tops.append(jnp.where(here, float(b), 0.0).astype(BF16))
            lows.append(jnp.where(here, place, 0.0).astype(BF16))
        both = jnp.concatenate([jnp.concatenate(tops, axis=1), jnp.concatenate(lows, axis=1)], axis=0)
        found = lax.dot_general(both, hot[...], (((1,), (1,)), ((), ())), preferred_element_type=F32).astype(I32)
        block_back[...] = found[0:nb]
        spread(found[nb : 2 * nb], hot_back)

    def launch(e):
        near = nears[e]
        sums = [jnp.zeros((SUB, BLK), F32), jnp.zeros((SUB, BLK), F32)]
        for b in range(nb):
            x = xs[b]
            near[1, b] = x
            for k in range(2):
                sums[k] = sums[k] + ws[k, b] * x
        parts[e, me] = sums[0] + pltpu.roll(sums[1], 3, 0)
        part_copies = []
        for at, target in enumerate(others):
            copy = pltpu.make_async_remote_copy(
                src_ref=parts.at[e, me],
                dst_ref=parts.at[e, me],
                send_sem=part_send.at[e, at],
                recv_sem=part_recv.at[e, at],
                device_id=target,
                device_id_type=MESH,
            )
            copy.start()
            part_copies.append(copy)
        halo = neighbours(near, halo_send.at[e], halo_recv.at[e])
        send_both(*halo)
        return part_copies, halo

    def whole(tile, first):
        return jnp.sum(tile[first : first + 3, :], axis=(0, 1), keepdims=True)

    def settle(e, part_copies, before, crossed):
        for copy in part_copies:
            copy.wait()
        total = parts[e, 0]
        for d in range(1, doms):
            total = total + parts[e, d]
        pulls = []
        for k in range(2):
            collective = whole(total, 3 * k)
            if before is not None:
                collective = collective - before[0] * crossed[k] - before[1] * crossed[k + 1]
            pulls.append(stiff_s[k] * (collective - centres[k][:, 0:1]))
        return pulls

    def pairs(e, halo, before, meanwhile):
        near = nears[e]

        def features(slab, b, value):
            value = value * SCALE
            high = value.astype(BF16).astype(F32)
            middle = (value - high).astype(BF16).astype(F32)
            kept = high + middle
            square = jnp.where(three, kept * kept, 0.0)
            norm = jnp.broadcast_to(-0.5 * jnp.sum(square, axis=0, keepdims=True), (SUB, BLK))
            one = norm.astype(BF16).astype(F32)
            two = (norm - one).astype(BF16).astype(F32)
            norms = jnp.where(lines == 3, one, jnp.where(lines == 4, two, jnp.where(lines == 5, norm - one - two, 0.0)))
            units = jnp.where((lines >= 3) & (lines < 6), 1.0, 0.0)
            counted = jnp.where(lines == 6, 1.0, 0.0)
            plain = jnp.where(three, high, 0.0)
            fine = jnp.where(three, middle, 0.0)
            theirs = jnp.concatenate([plain + norms + counted, fine + units, plain, fine], axis=0)
            lines_of[slab * nb + b] = theirs[0 : 2 * SUB, :].astype(BF16)
            turned_of[slab * nb + b] = jnp.transpose(theirs).astype(BF16)
            return kept, plain + units, plain + norms, fine

        for b in range(nb):
            kept, top, second_top, fine = features(1, b, xs[b])
            held[b] = kept
            own_of[b] = jnp.concatenate([top, second_top, fine, fine], axis=0).astype(BF16)

        meanwhile()

        wait_both(*halo)
        for b in range(nb):
            for slab in (0, 2):
                value = near[slab, b]
                if before is not None:
                    value = value - before[0] * near_w[slab, 0, b] - before[1] * near_w[slab, 1, b]
                features(slab, b, value)

        def ours(p):
            return jnp.clip(list_s[0, p], 0, nb - 1)

        def their(p):
            return jnp.clip(list_s[1, p], 0, 3 * nb - 1)

        def first_of(p):
            return jnp.dot(turned_of[their(p)], own_of[ours(p)], preferred_element_type=F32)

        def second_of(p, carried, logits):
            pieces = [split2(jnp.exp2(logit)) for logit in logits]
            lines_at = [lines_of[their(p + u)] for u in range(2)]
            pulled = jnp.dot(
                jnp.concatenate([jnp.concatenate([line, line], axis=1) for line in lines_at], axis=0),
                jnp.concatenate([jnp.concatenate([pieces[0][h], pieces[1][h]], axis=1) for h in range(2)], axis=0),
                preferred_element_type=F32,
            )
            for u in range(2):
                at = slice(u * BLK, (u + 1) * BLK)
                tile = pulled[2 * u * SUB : (2 * u + 1) * SUB, at] + pulled[(2 * u + 1) * SUB : (2 * u + 2) * SUB, at]
                carried = carried * keep_s[2, p + u] + tile
                prefix[p + u + 1] = carried
            return carried

        def body(i, carried):
            start = i * UNROLL
            ready = [first_of(start + u) for u in range(GROUP)]
            for g in range(0, UNROLL, GROUP):
                later = [first_of(start + g + GROUP + u) for u in range(GROUP)] if g + GROUP < UNROLL else []
                for u in range(0, GROUP, 2):
                    carried = second_of(start + g + u, carried, ready[u : u + 2])
                ready = later
            return carried

        prefix[0] = jnp.zeros((SUB, BLK), F32)
        lax.fori_loop(0, slots // UNROLL, body, jnp.zeros((SUB, BLK), F32))

    def write(source, target):
        for b, line in moved(source[...].reshape(rows, BLK), hot_back, block_back):
            raw[b * SUB : (b + 1) * SUB, :] = line
        for c in range(3):
            target[c] = raw[pl.ds(c, nb, stride=SUB), :]

    def write_state():
        write(xs, out_x)
        write(vs, out_v)

    def pair_force(b):
        pulled = prefix[jnp.clip(list_s[2, b], 0, slots)]
        return (PAIR_EPS / SCALE) * (held[b] * jnp.broadcast_to(pulled[6:7, :], (SUB, BLK)) - pulled)

    part_copies, halo = launch(0)
    pairs(0, halo, None, take_velocities)
    before = crossed = None
    for step in range(STEPS):
        kick = 1.0 if step == 0 else 2.0
        for b in range(nb):
            pair = pair_force(b)
            fs[b] = pair
            xs[b] = xs[b] + DT * (vs[b] + kick * half_m[b] * pair)
        next_copies, halo = launch(step + 1)
        pulls = settle(step, part_copies, before, crossed)
        before = [jnp.broadcast_to(kick * pull, (SUB, BLK)) for pull in pulls]
        for b in range(nb):
            vs[b] = vs[b] + kick * half_m[b] * (fs[b] - pulls[0] * ws[0, b] - pulls[1] * ws[1, b])
            xs[b] = xs[b] - before[0] * near_w[1, 0, b] - before[1] * near_w[1, 1, b]
        before_sum = [kick * pull for pull in pulls]

        def meanwhile():
            if step == 0:
                wait_both(*weight_halo)
                invert()
            if step == STEPS - 1:
                write_state()

        if step == 0:
            for copy in early:
                copy.wait()
            total = cross_parts[0]
            last = cross_last[0]
            for d in range(1, doms):
                total = total + cross_parts[d]
                last = last + cross_last[d]
            crossed = [whole(total, 0), whole(total, 3), whole(last, 0)]
        pairs(step + 1, halo, before, meanwhile)
        before = before_sum
        part_copies = next_copies
    pulls = settle(STEPS, part_copies, before, crossed)
    for b in range(nb):
        fs[b] = pair_force(b) - pulls[0] * ws[0, b] - pulls[1] * ws[1, b]
    write(fs, out_f)


def finish(mass, x, v, f, out_x, out_v, out_f):
    out_x[...] = x[...]
    out_f[...] = f[...]
    out_v[...] = v[...] + (0.5 * DT) * mass[...][None] * f[...]


def per_device(
    positions, velocities, inv_mass, cv_weight, stiffness, centers, block_order, pair_count, pair_own, pair_other,
    accept_row, accept_col,
):
    atoms = block_order.shape[0]
    nb = atoms // BLK
    slots = pair_own.shape[1]
    doms = lax.axis_size("dom")
    evals = STEPS + 1
    wide = BLK * pl.cdiv(slots, BLK)
    vmem = pl.BlockSpec(memory_space=pltpu.VMEM)
    dma = pltpu.SemaphoreType.DMA
    shape = jax.ShapeDtypeStruct((3, nb, BLK), F32)
    state = pltpu.VMEM((nb, SUB, BLK), F32)
    weights = cv_weight.transpose(1, 0, 2).reshape(3, 2, nb, BLK).transpose(0, 2, 1, 3).reshape(6 * nb, BLK)
    outs = pl.pallas_call(
        functools.partial(kernel, (doms, nb, slots)),
        out_shape=(shape, shape, shape),
        in_specs=[pl.BlockSpec(memory_space=pl.ANY)] * 12,
        out_specs=(vmem, vmem, vmem),
        scratch_shapes=[
            pltpu.VMEM((3, nb, BLK), F32),
            pltpu.VMEM((3, nb, BLK), F32),
            pltpu.VMEM((nb, BLK), F32),
            pltpu.VMEM((6 * nb, BLK), F32),
            pltpu.VMEM((nb, BLK), I32),
            pltpu.VMEM((1, slots), I32),
            pltpu.VMEM((1, slots), I32),
            pltpu.SMEM((1,), I32),
            pltpu.SMEM((2,), F32),
            pltpu.SMEM((1, 2), F32),
            pltpu.SMEM((1, 1), I32),
            pltpu.SMEM((1, 1), I32),
            dma((12,)),
            pltpu.VMEM((BLK, atoms), BF16),
            pltpu.VMEM((BLK, atoms), BF16),
            pltpu.VMEM((nb, BLK), I32),
            pltpu.VMEM((nb, BLK), I32),
            pltpu.VMEM((nb * SUB, BLK), F32),
            pltpu.VMEM((nb * SUB, BLK), F32),
            pltpu.VMEM((3, 3, nb, BLK), F32),
            pltpu.VMEM((3, 3, nb, BLK), F32),
            pltpu.VMEM((3, SUB, BLK), F32),
            pltpu.VMEM((SUB, BLK), F32),
            pltpu.VMEM((evals, doms, SUB, BLK), F32),
            pltpu.VMEM((slots + 1, SUB, BLK), F32),
            pltpu.VMEM((3 * nb, 2 * SUB, BLK), BF16),
            pltpu.VMEM((3 * nb, BLK, 4 * SUB), BF16),
            pltpu.VMEM((nb, 4 * SUB, BLK), BF16),
            pltpu.VMEM((SUB, wide), I32),
            pltpu.VMEM((SUB, wide), F32),
            pltpu.SMEM((SUB, wide), I32),
            pltpu.SMEM((SUB, wide), F32),
            state, state, state, state, state,
            pltpu.VMEM((2, nb, SUB, BLK), F32),
            pltpu.VMEM((3, 2, nb, SUB, BLK), F32),
            pltpu.VMEM((doms, SUB, BLK), F32),
            pltpu.VMEM((doms, SUB, BLK), F32),
            dma((3,)), dma((3,)), dma((3,)), dma((3,)), dma((3,)), dma((3,)),
            dma((evals, 2)), dma((evals, 2)), dma((evals, doms)), dma((evals, doms)), dma((2,)),
            dma((2,)), dma((2,)), dma((2, doms)), dma((2, doms)),
        ]
        + [pltpu.VMEM((3, nb, SUB, BLK), F32)] * evals,
        compiler_params=pltpu.CompilerParams(collective_id=0, has_side_effects=True),
        name="windows",
    )(
        positions.reshape(3, nb, BLK), velocities.reshape(3, nb, BLK), inv_mass.reshape(nb, BLK), weights, block_order.reshape(nb, BLK), pair_own,
        pair_other, pair_count, stiffness, centers[0], accept_row, accept_col,
    )
    outs = pl.pallas_call(
        finish,
        out_shape=(shape, shape, shape),
        in_specs=[vmem] * 4,
        out_specs=(vmem, vmem, vmem),
        name="finish",
    )(inv_mass.reshape(nb, BLK), *outs)
    return tuple(out.reshape(1, 1, 3, atoms) for out in outs)


def solution(mesh):
    placed = (
        P("wrow", "wcol", None, "dom"),
        P("wrow", "wcol", None, "dom"),
        P("dom"),
        P(None, None, "dom"),
        P(),
        P("wrow", "wcol", None),
        P("dom"),
        P("dom"),
        P("dom", None),
        P("dom", None),
        P("wrow", "wcol"),
        P("wrow", "wcol"),
    )
    return jax.shard_map(
        per_device,
        mesh=mesh,
        in_specs=placed,
        out_specs=(
            P("wrow", "wcol", None, "dom"),
            P("wrow", "wcol", None, "dom"),
            P("wrow", "wcol", None, "dom"),
        ),
        check_vma=False,
    )
```

```python
import functools
import math

import jax
import jax.numpy as jnp
from jax import lax
from jax.experimental import pallas as pl
from jax.experimental.pallas import tpu as pltpu
from jax.sharding import PartitionSpec as P

BLK = 128
SUB = 8
STEPS = 3
PAIR_EPS = 0.015625
DT = 0.1
SCALE = math.sqrt(math.log2(math.e))
GROUP = 8
UNROLL = 64
MESH = pl.DeviceIdType.MESH
F32 = jnp.float32
BF16 = jnp.bfloat16
I32 = jnp.int32


def split2(value):
    high = value.astype(BF16)
    return high, (value - high.astype(F32)).astype(BF16)


def kernel(
    sizes,
    pos_h, vel_h, mass_h, cvw_h, order_h, own_h, other_h, count_h, stiff_h, centers_h, arow_h, acol_h,
    out_x, out_v, out_f,
    pos, vel, mass, cvw, order, own_row, other_row, count_s, stiff_s, centers_s, arow_s, acol_s, in_sem,
    hot, hot_back, block_of, block_back, raw, raw_w, got_x, got_v, got_aux, aux, parts, prefix, lines_of, turned_of, own_of,
    table_i, table_f, list_s, keep_s, xs, vs, fs, held, half_m, ws, near_w, cross_parts, cross_last, done, given,
    sx_send, sx_recv, sv_send, sv_recv, sa_send, sa_recv, halo_send, halo_recv, part_send, part_recv, list_sem, weight_send, weight_recv, cross_send, cross_recv, home_send, home_recv, *nears,
):
    doms, nb, slots = sizes
    rows = nb * SUB
    row = lax.axis_index("wrow")
    col = lax.axis_index("wcol")
    me = lax.axis_index("dom")
    row_to = row + 1 - 2 * lax.rem(row, 2)
    col_to = col + 1 - 2 * lax.rem(col, 2)
    partners = [(row_to, col, me), (row, col_to, me), (row_to, col_to, me)]
    odd = lax.rem(me, 2)

    def row_at(slab):
        return row + (row_to - row) * lax.rem(me + slab, 2)

    others = []
    for off in range(1, doms):
        slab = lax.rem(me + off, doms)
        others.append((row_at(slab), col, slab))

    barrier = pltpu.get_barrier_semaphore()
    for target in partners + others:
        pl.semaphore_signal(barrier, inc=1, device_id=target, device_id_type=MESH)
    entered = [
        pltpu.make_async_copy(source, target, in_sem.at[at])
        for at, (source, target) in enumerate((
            (centers_h, centers_s), (arow_h, arow_s), (acol_h, acol_s), (pos_h, pos), (vel_h, vel), (order_h, order), (cvw_h, cvw), (mass_h, mass),
            (own_h, own_row), (other_h, other_row), (count_h, count_s), (stiff_h, stiff_s),
        ))
    ]
    for copy in entered:
        copy.start()
    for copy in entered[0:5]:
        copy.wait()
    lines = lax.broadcasted_iota(I32, (SUB, BLK), 0)
    aux[...] = jnp.where(
        lines == 0,
        centers_s[0, 0],
        jnp.where(
            lines == 1, centers_s[0, 1], jnp.where(lines == 2, arow_s[0, 0].astype(F32), acol_s[0, 0].astype(F32))
        ),
    )
    pl.semaphore_wait(barrier, len(partners) + len(others))

    def exchange(source, target, sends, recvs):
        copies = []
        for at, partner in enumerate(partners):
            copy = pltpu.make_async_remote_copy(
                src_ref=source,
                dst_ref=target.at[at],
                send_sem=sends.at[at],
                recv_sem=recvs.at[at],
                device_id=partner,
                device_id_type=MESH,
            )
            copy.start()
            copies.append(copy)
        return copies

    aux_copies = exchange(aux, got_aux, sa_send, sa_recv)
    x_copies = exchange(pos, got_x, sx_send, sx_recv)
    v_copies = exchange(vel, got_v, sv_send, sv_recv)

    for copy in entered[5:]:
        copy.wait()
    lane_line = lax.broadcasted_iota(I32, (BLK, BLK), 0)

    def spread(low, target):
        for b in range(nb):
            target[:, b * BLK : (b + 1) * BLK] = jnp.where(low[b : b + 1, :] == lane_line, 1.0, 0.0).astype(BF16)

    listed = order[...]
    block_of[...] = lax.div(listed, BLK)
    spread(lax.rem(listed, BLK), hot)

    def moved(source, hots, blocks):
        left = jnp.concatenate(split2(source), axis=1)
        for b in range(0, nb, 2):
            right = hots[:, b * BLK : (b + 2) * BLK]
            got = jnp.dot(left, jnp.concatenate([right, right], axis=0), preferred_element_type=F32)
            for u in range(2):
                home = jnp.broadcast_to(blocks[b + u : b + u + 1, :], (SUB, BLK))
                line = got[0:SUB, u * BLK : (u + 1) * BLK]
                for s in range(1, nb):
                    line = jnp.where(home == s, got[s * SUB : (s + 1) * SUB, u * BLK : (u + 1) * BLK], line)
                yield b + u, line

    raw[...] = jnp.zeros((rows, BLK), F32)
    raw_w[...] = jnp.zeros((rows, BLK), F32)
    for k in range(2):
        for c in range(3):
            raw_w[pl.ds(3 * k + c, nb, stride=SUB), :] = cvw[pl.ds(2 * nb * c + k, nb, stride=2), :]
    raw_w[pl.ds(6, nb, stride=SUB), :] = mass[...]
    three = lines < 3
    for b, line in moved(raw_w[...], hot, block_of):
        ws[0, b] = jnp.where(three, line, 0.0)
        ws[1, b] = jnp.where(three, pltpu.roll(line, SUB - 3, 0), 0.0)
        half_m[b] = jnp.where(three, (0.5 * DT) * jnp.broadcast_to(line[6:7, :], (SUB, BLK)), 0.0)
    cross = [jnp.zeros((SUB, BLK), F32) for _ in range(3)]
    for b in range(nb):
        for k in range(2):
            shift = DT * half_m[b] * ws[k, b]
            near_w[1, k, b] = shift
            for j in range(k, 2):
                cross[k + j] = cross[k + j] + shift * ws[j, b]
    cross_parts[me] = cross[0] + pltpu.roll(cross[1], 3, 0)
    cross_last[me] = cross[2]
    early = []
    for at, target in enumerate(others):
        for which, held_parts in enumerate((cross_parts, cross_last)):
            copy = pltpu.make_async_remote_copy(
                src_ref=held_parts.at[me],
                dst_ref=held_parts.at[me],
                send_sem=cross_send.at[which, at],
                recv_sem=cross_recv.at[which, at],
                device_id=target,
                device_id_type=MESH,
            )
            copy.start()
            early.append(copy)

    def neighbours(ref, sends, recvs):
        source = ref.at[1, ..., 0:3, :]
        return tuple(
            pltpu.make_async_remote_copy(
                src_ref=source,
                dst_ref=ref.at[1 - step, ..., 0:3, :],
                send_sem=sends.at[at],
                recv_sem=recvs.at[at],
                device_id=(row_to, col, lax.rem(me + doms + step, doms)),
                device_id_type=MESH,
            )
            for at, step in enumerate((1, -1))
        )

    def send_both(up, down):
        @pl.when(me < doms - 1)
        def _():
            up.start()

        @pl.when(me > 0)
        def _():
            down.start()

    def wait_both(up, down):
        @pl.when(me < doms - 1)
        def _():
            up.wait_send()
            down.wait_recv()

        @pl.when(me > 0)
        def _():
            down.wait_send()
            up.wait_recv()

    weight_halo = neighbours(near_w, weight_send, weight_recv)
    send_both(*weight_halo)

    slot_lane = lax.broadcasted_iota(I32, (1, slots), 1)
    live = slot_lane < count_s[0]
    owner = jnp.where(live, own_row[...], nb).astype(F32)
    first = lax.broadcasted_iota(I32, (slots, slots), 0)
    second = lax.broadcasted_iota(I32, (slots, slots), 1)
    square = jnp.broadcast_to(owner, (slots, slots))
    unit = jnp.where(first == second, 1.0, 0.0).astype(BF16)
    turned = lax.dot_general(unit, square.astype(BF16), (((1,), (1,)), ((), ())), preferred_element_type=F32)
    ahead = jnp.where((turned == square) & (first < second), 1.0, 0.0)
    earlier = jnp.sum(ahead, axis=0, keepdims=True)
    rank = earlier + jnp.sum(jnp.where(turned < square, 1.0, 0.0), axis=0, keepdims=True)
    chosen_slot = jnp.where(jnp.broadcast_to(rank, (slots, slots)) == first.astype(F32), 1.0, 0.0).astype(BF16)
    list_line = lax.broadcasted_iota(I32, (SUB, slots), 0)
    lists = jnp.where(
        list_line == 0,
        jnp.where(owner < nb, owner, 0.0),
        jnp.where(list_line == 1, other_row[...].astype(F32), jnp.where(earlier > 0.0, 1.0, 0.0)),
    )
    ordered = lax.dot_general(lists.astype(BF16), chosen_slot, (((1,), (1,)), ((), ())), preferred_element_type=F32)
    upto = jnp.sum(jnp.where(turned <= second.astype(F32), 1.0, 0.0), axis=0, keepdims=True)
    some = jnp.sum(jnp.where(turned == second.astype(F32), 1.0, 0.0), axis=0, keepdims=True)
    table_f[...] = jnp.zeros(table_f.shape, F32)
    table_i[...] = jnp.zeros(table_i.shape, I32)
    table_f[:, 0:slots] = ordered
    table_i[:, 0:slots] = jnp.where(list_line == 2, jnp.where(some > 0.0, upto, 0.0), ordered).astype(I32)
    list_copies = [
        pltpu.make_async_copy(table_i, list_s, list_sem.at[0]),
        pltpu.make_async_copy(table_f, keep_s, list_sem.at[1]),
    ]
    for copy in list_copies:
        copy.start()

    for copy in aux_copies:
        copy.wait()
    take_row = jnp.full((SUB, BLK), arow_s[0, 0].astype(F32)) > 0.5
    swap = jnp.full((SUB, BLK), odd) > 0
    col_flag = jnp.where(
        swap, jnp.broadcast_to(got_aux[0, 3:4, :], (SUB, BLK)), jnp.broadcast_to(aux[3:4, :], (SUB, BLK))
    )
    take_col = col_flag > 0.5
    take_far = jnp.broadcast_to(got_aux[1, 2:3, :], (SUB, BLK)) > 0.5

    def chosen(mine, by_row, by_col, by_both):
        mine, by_row = jnp.where(swap, by_row, mine), jnp.where(swap, mine, by_row)
        by_col, by_both = jnp.where(swap, by_both, by_col), jnp.where(swap, by_col, by_both)
        far = jnp.where(take_far, by_both, by_col)
        close = jnp.where(take_row, by_row, mine)
        return jnp.where(take_col, far, close)

    centre = chosen(aux[...], got_aux[0], got_aux[1], got_aux[2])
    centres = [centre[0:1, :], centre[1:2, :]]

    def take_window(source, got):
        for c in range(3):
            for b in range(0, nb, SUB):
                raw[pl.ds(b * SUB + c, SUB, stride=SUB), :] = chosen(
                    source[c, b : b + SUB], got[0, c, b : b + SUB], got[1, c, b : b + SUB], got[2, c, b : b + SUB]
                )

    for copy in x_copies:
        copy.wait()
    take_window(pos, got_x)
    for b, line in moved(raw[...], hot, block_of):
        xs[b] = line

    def take_velocities():
        for copy in list_copies:
            copy.wait()
        for copy in v_copies:
            copy.wait()
        take_window(vel, got_v)
        for b, line in moved(raw[...], hot, block_of):
            vs[b] = line

    def invert():
        block_line = lax.broadcasted_iota(I32, (nb, BLK), 0)
        place = lax.broadcasted_iota(I32, (nb, BLK), 1).astype(F32)
        tops, lows = [], []
        for b in range(nb):
            here = block_of[b : b + 1, :] == block_line
            tops.append(jnp.where(here, float(b), 0.0).astype(BF16))
            lows.append(jnp.where(here, place, 0.0).astype(BF16))
        both = jnp.concatenate([jnp.concatenate(tops, axis=1), jnp.concatenate(lows, axis=1)], axis=0)
        found = lax.dot_general(both, hot[...], (((1,), (1,)), ((), ())), preferred_element_type=F32).astype(I32)
        block_back[...] = found[0:nb]
        spread(found[nb : 2 * nb], hot_back)

    def launch(e):
        near = nears[e]
        sums = [jnp.zeros((SUB, BLK), F32), jnp.zeros((SUB, BLK), F32)]
        for b in range(nb):
            x = xs[b]
            near[1, b] = x
            for k in range(2):
                sums[k] = sums[k] + ws[k, b] * x
        parts[e, me] = sums[0] + pltpu.roll(sums[1], 3, 0)
        part_copies = []
        for at, target in enumerate(others):
            copy = pltpu.make_async_remote_copy(
                src_ref=parts.at[e, me],
                dst_ref=parts.at[e, me],
                send_sem=part_send.at[e, at],
                recv_sem=part_recv.at[e, at],
                device_id=target,
                device_id_type=MESH,
            )
            copy.start()
            part_copies.append(copy)
        halo = neighbours(near, halo_send.at[e], halo_recv.at[e])
        send_both(*halo)
        return part_copies, halo

    def whole(tile, first):
        return jnp.sum(tile[first : first + 3, :], axis=(0, 1), keepdims=True)

    def settle(e, part_copies, before, crossed):
        for copy in part_copies:
            copy.wait()
        total = parts[e, 0]
        for d in range(1, doms):
            total = total + parts[e, d]
        pulls = []
        for k in range(2):
            collective = whole(total, 3 * k)
            if before is not None:
                collective = collective - before[0] * crossed[k] - before[1] * crossed[k + 1]
            pulls.append(stiff_s[k] * (collective - centres[k][:, 0:1]))
        return pulls

    def pairs(e, halo, before, meanwhile):
        near = nears[e]

        def features(slab, b, value):
            value = value * SCALE
            high = value.astype(BF16).astype(F32)
            middle = (value - high).astype(BF16).astype(F32)
            kept = high + middle
            square = jnp.where(three, kept * kept, 0.0)
            norm = jnp.broadcast_to(-0.5 * jnp.sum(square, axis=0, keepdims=True), (SUB, BLK))
            one = norm.astype(BF16).astype(F32)
            two = (norm - one).astype(BF16).astype(F32)
            norms = jnp.where(lines == 3, one, jnp.where(lines == 4, two, jnp.where(lines == 5, norm - one - two, 0.0)))
            units = jnp.where((lines >= 3) & (lines < 6), 1.0, 0.0)
            counted = jnp.where(lines == 6, 1.0, 0.0)
            plain = jnp.where(three, high, 0.0)
            fine = jnp.where(three, middle, 0.0)
            theirs = jnp.concatenate([plain + norms + counted, fine + units, plain, fine], axis=0)
            lines_of[slab * nb + b] = theirs[0 : 2 * SUB, :].astype(BF16)
            turned_of[slab * nb + b] = jnp.transpose(theirs).astype(BF16)
            return kept, plain + units, plain + norms, fine

        for b in range(nb):
            kept, top, second_top, fine = features(1, b, xs[b])
            held[b] = kept
            own_of[b] = jnp.concatenate([top, second_top, fine, fine], axis=0).astype(BF16)

        meanwhile()

        wait_both(*halo)
        for b in range(nb):
            for slab in (0, 2):
                value = near[slab, b]
                if before is not None:
                    value = value - before[0] * near_w[slab, 0, b] - before[1] * near_w[slab, 1, b]
                features(slab, b, value)

        def ours(p):
            return jnp.clip(list_s[0, p], 0, nb - 1)

        def their(p):
            return jnp.clip(list_s[1, p], 0, 3 * nb - 1)

        def first_of(p):
            return jnp.dot(turned_of[their(p)], own_of[ours(p)], preferred_element_type=F32)

        def second_of(p, carried, logits):
            pieces = [split2(jnp.exp2(logit)) for logit in logits]
            lines_at = [lines_of[their(p + u)] for u in range(2)]
            pulled = jnp.dot(
                jnp.concatenate([jnp.concatenate([line, line], axis=1) for line in lines_at], axis=0),
                jnp.concatenate([jnp.concatenate([pieces[0][h], pieces[1][h]], axis=1) for h in range(2)], axis=0),
                preferred_element_type=F32,
            )
            for u in range(2):
                at = slice(u * BLK, (u + 1) * BLK)
                tile = pulled[2 * u * SUB : (2 * u + 1) * SUB, at] + pulled[(2 * u + 1) * SUB : (2 * u + 2) * SUB, at]
                carried = carried * keep_s[2, p + u] + tile
                prefix[p + u + 1] = carried
            return carried

        def body(i, carried):
            start = i * UNROLL
            ready = [first_of(start + u) for u in range(GROUP)]
            for g in range(0, UNROLL, GROUP):
                later = [first_of(start + g + GROUP + u) for u in range(GROUP)] if g + GROUP < UNROLL else []
                for u in range(0, GROUP, 2):
                    carried = second_of(start + g + u, carried, ready[u : u + 2])
                ready = later
            return carried

        prefix[0] = jnp.zeros((SUB, BLK), F32)
        lax.fori_loop(0, slots // UNROLL, body, jnp.zeros((SUB, BLK), F32))

    def write(source, at):
        for b, line in moved(source[...].reshape(rows, BLK), hot_back, block_back):
            raw[b * SUB : (b + 1) * SUB, :] = line
        for c in range(3):
            done[at, c] = raw[pl.ds(c, nb, stride=SUB), :]
        copy = pltpu.make_async_remote_copy(
            src_ref=done.at[at],
            dst_ref=given.at[at],
            send_sem=home_send.at[at],
            recv_sem=home_recv.at[at],
            device_id=partners[0],
            device_id_type=MESH,
        )

        @pl.when(odd == 1)
        def _():
            copy.start()

        return copy

    homes = []

    def write_state():
        homes.append(write(xs, 0))
        homes.append(write(vs, 1))

    def pair_force(b):
        pulled = prefix[jnp.clip(list_s[2, b], 0, slots)]
        return (PAIR_EPS / SCALE) * (held[b] * jnp.broadcast_to(pulled[6:7, :], (SUB, BLK)) - pulled)

    part_copies, halo = launch(0)
    pairs(0, halo, None, take_velocities)
    before = crossed = None
    for step in range(STEPS):
        kick = 1.0 if step == 0 else 2.0
        for b in range(nb):
            pair = pair_force(b)
            fs[b] = pair
            xs[b] = xs[b] + DT * (vs[b] + kick * half_m[b] * pair)
        next_copies, halo = launch(step + 1)
        pulls = settle(step, part_copies, before, crossed)
        before = [jnp.broadcast_to(kick * pull, (SUB, BLK)) for pull in pulls]
        for b in range(nb):
            vs[b] = vs[b] + kick * half_m[b] * (fs[b] - pulls[0] * ws[0, b] - pulls[1] * ws[1, b])
            xs[b] = xs[b] - before[0] * near_w[1, 0, b] - before[1] * near_w[1, 1, b]
        before_sum = [kick * pull for pull in pulls]

        def meanwhile():
            if step == 0:
                wait_both(*weight_halo)
                invert()
            if step == STEPS - 1:
                write_state()

        if step == 0:
            for copy in early:
                copy.wait()
            total = cross_parts[0]
            last = cross_last[0]
            for d in range(1, doms):
                total = total + cross_parts[d]
                last = last + cross_last[d]
            crossed = [whole(total, 0), whole(total, 3), whole(last, 0)]
        pairs(step + 1, halo, before, meanwhile)
        before = before_sum
        part_copies = next_copies
    pulls = settle(STEPS, part_copies, before, crossed)
    for b in range(nb):
        fs[b] = pair_force(b) - pulls[0] * ws[0, b] - pulls[1] * ws[1, b]
    homes.append(write(fs, 2))

    @pl.when(odd == 0)
    def _():
        for at, out in enumerate((out_x, out_v, out_f)):
            out[...] = done[at]

    @pl.when(odd == 1)
    def _():
        for copy, at, out in zip(homes, range(3), (out_x, out_v, out_f)):
            copy.wait()
            out[...] = given[at]


def finish(mass, x, v, f, out_x, out_v, out_f):
    out_x[...] = x[...]
    out_f[...] = f[...]
    out_v[...] = v[...] + (0.5 * DT) * mass[...][None] * f[...]


def per_device(
    positions, velocities, inv_mass, cv_weight, stiffness, centers, block_order, pair_count, pair_own, pair_other,
    accept_row, accept_col,
):
    atoms = block_order.shape[0]
    nb = atoms // BLK
    slots = pair_own.shape[1]
    doms = lax.axis_size("dom")
    evals = STEPS + 1
    wide = BLK * pl.cdiv(slots, BLK)
    vmem = pl.BlockSpec(memory_space=pltpu.VMEM)
    dma = pltpu.SemaphoreType.DMA
    shape = jax.ShapeDtypeStruct((3, nb, BLK), F32)
    state = pltpu.VMEM((nb, SUB, BLK), F32)
    weights = cv_weight.transpose(1, 0, 2).reshape(3, 2, nb, BLK).transpose(0, 2, 1, 3).reshape(6 * nb, BLK)
    outs = pl.pallas_call(
        functools.partial(kernel, (doms, nb, slots)),
        out_shape=(shape, shape, shape),
        in_specs=[pl.BlockSpec(memory_space=pl.ANY)] * 12,
        out_specs=(vmem, vmem, vmem),
        scratch_shapes=[
            pltpu.VMEM((3, nb, BLK), F32),
            pltpu.VMEM((3, nb, BLK), F32),
            pltpu.VMEM((nb, BLK), F32),
            pltpu.VMEM((6 * nb, BLK), F32),
            pltpu.VMEM((nb, BLK), I32),
            pltpu.VMEM((1, slots), I32),
            pltpu.VMEM((1, slots), I32),
            pltpu.SMEM((1,), I32),
            pltpu.SMEM((2,), F32),
            pltpu.SMEM((1, 2), F32),
            pltpu.SMEM((1, 1), I32),
            pltpu.SMEM((1, 1), I32),
            dma((12,)),
            pltpu.VMEM((BLK, atoms), BF16),
            pltpu.VMEM((BLK, atoms), BF16),
            pltpu.VMEM((nb, BLK), I32),
            pltpu.VMEM((nb, BLK), I32),
            pltpu.VMEM((nb * SUB, BLK), F32),
            pltpu.VMEM((nb * SUB, BLK), F32),
            pltpu.VMEM((3, 3, nb, BLK), F32),
            pltpu.VMEM((3, 3, nb, BLK), F32),
            pltpu.VMEM((3, SUB, BLK), F32),
            pltpu.VMEM((SUB, BLK), F32),
            pltpu.VMEM((evals, doms, SUB, BLK), F32),
            pltpu.VMEM((slots + 1, SUB, BLK), F32),
            pltpu.VMEM((3 * nb, 2 * SUB, BLK), BF16),
            pltpu.VMEM((3 * nb, BLK, 4 * SUB), BF16),
            pltpu.VMEM((nb, 4 * SUB, BLK), BF16),
            pltpu.VMEM((SUB, wide), I32),
            pltpu.VMEM((SUB, wide), F32),
            pltpu.SMEM((SUB, wide), I32),
            pltpu.SMEM((SUB, wide), F32),
            state, state, state, state, state,
            pltpu.VMEM((2, nb, SUB, BLK), F32),
            pltpu.VMEM((3, 2, nb, SUB, BLK), F32),
            pltpu.VMEM((doms, SUB, BLK), F32),
            pltpu.VMEM((doms, SUB, BLK), F32),
            pltpu.VMEM((3, 3, nb, BLK), F32),
            pltpu.VMEM((3, 3, nb, BLK), F32),
            dma((3,)), dma((3,)), dma((3,)), dma((3,)), dma((3,)), dma((3,)),
            dma((evals, 2)), dma((evals, 2)), dma((evals, doms)), dma((evals, doms)), dma((2,)),
            dma((2,)), dma((2,)), dma((2, doms)), dma((2, doms)), dma((3,)), dma((3,)),
        ]
        + [pltpu.VMEM((3, nb, SUB, BLK), F32)] * evals,
        compiler_params=pltpu.CompilerParams(collective_id=0, has_side_effects=True),
        name="windows",
    )(
        positions.reshape(3, nb, BLK), velocities.reshape(3, nb, BLK), inv_mass.reshape(nb, BLK), weights, block_order.reshape(nb, BLK), pair_own,
        pair_other, pair_count, stiffness, centers[0], accept_row, accept_col,
    )
    outs = pl.pallas_call(
        finish,
        out_shape=(shape, shape, shape),
        in_specs=[vmem] * 4,
        out_specs=(vmem, vmem, vmem),
        name="finish",
    )(inv_mass.reshape(nb, BLK), *outs)
    return tuple(out.reshape(1, 1, 3, atoms) for out in outs)


def solution(mesh):
    placed = (
        P("wrow", "wcol", None, "dom"),
        P("wrow", "wcol", None, "dom"),
        P("dom"),
        P(None, None, "dom"),
        P(),
        P("wrow", "wcol", None),
        P("dom"),
        P("dom"),
        P("dom", None),
        P("dom", None),
        P("wrow", "wcol"),
        P("wrow", "wcol"),
    )
    return jax.shard_map(
        per_device,
        mesh=mesh,
        in_specs=placed,
        out_specs=(
            P("wrow", "wcol", None, "dom"),
            P("wrow", "wcol", None, "dom"),
            P("wrow", "wcol", None, "dom"),
        ),
        check_vma=False,
    )
```
